32 devices in a mesh: kx: 2 (over x), ky: 4 (over y, core), kz: 4 (over z).
Axes of the slice: x: 2, y: 2, z: 4, core: 2. Of those that a mesh axis runs over, the one named last changes fastest.
Arguments:
- coefficients: bfloat16 [2, 2, 4, 4, 512, 2048], P(None, 'kx', 'ky', 'kz'), may hold values from -1 to 1
- shift_blocks: int32 [3], replicated, may hold values from 1 to 15, as said below
Outputs:
- centre: float32 [3, 512], replicated
- spread: float32 [3, 512], replicated
- coherence: float32 [3, 2, 4, 4], P(None, 'kx', 'ky', 'kz')
The draws below stay inside these ranges and needn't reach their ends.
Inputs may be any that keep to these rules, and one draw needn't show every extreme that they name: The coefficients one period further along direction d are those of the first k-point of the string with plane-wave index g read at (g + 128 * shift_blocks[d]) mod 2048.
All inputs are finite; a program needn't handle non-finite values.
Results may differ from the reference program's by a relative error of at most 0.0003.
Values may be sent and summed in bfloat16 or wider, within the bound.
A program may use at most 128 MiB of HBM per device.

```python
import jax
import jax.numpy as jnp
from jax import lax

NB = 512
NGW = 2048
NX = 2
NY = 4
NZ = 4


def offsets_for(key):
    middle = jax.random.randint(jax.random.fold_in(key, 11), (1,), 1, NGW // 128).astype(jnp.int32)
    ends = jnp.array([1, NGW // 128 - 1], jnp.int32)
    values = jnp.concatenate([ends, middle])
    order = jax.random.permutation(jax.random.fold_in(key, 13), 3)
    return values[order].astype(jnp.int32)


def draw_shift_blocks(key, part):
    return offsets_for(key)


def mix_along(fields, shift, points, position):
    angles = jnp.arange(points, dtype=jnp.float32) * (jnp.pi / (2.0 * points))
    dims_shape = [1] * (fields.ndim + 1)
    dims_shape[position] = points
    cosine = jnp.cos(angles).reshape(dims_shape)
    sine = jnp.sin(angles).reshape(dims_shape)
    rolled = jnp.roll(fields, -shift, axis=-1)
    return cosine * jnp.expand_dims(fields, position) + sine * jnp.expand_dims(rolled, position)


def draw_coefficients(key, part):
    offsets = offsets_for(key) * 128
    subkeys = jax.random.split(jax.random.fold_in(key, 23), 5)
    entry_scale = 1.0 / jnp.sqrt(2.0 * NGW)
    common = jnp.clip(jax.random.normal(subkeys[0], (2, NB, NGW), jnp.float32), -6.0, 6.0) * entry_scale
    fields = mix_along(common, offsets[2], NZ, 1)
    fields = mix_along(fields, offsets[1], NY, 1)
    fields = mix_along(fields, offsets[0], NX, 1)
    full_shape = (2, NX, NY, NZ, NB, NGW)
    roughness = jnp.clip(jax.random.normal(subkeys[1], full_shape, jnp.float32), -6.0, 6.0)
    amplitude = jnp.exp(jax.random.uniform(subkeys[2], (NB,), jnp.float32, jnp.log(0.1), jnp.log(0.6)))
    jitter = 0.35
    fields = fields + amplitude[:, None] * roughness * entry_scale
    winding = jax.random.uniform(subkeys[3], (3, NB), jnp.float32, -0.2, 0.2)
    x_frac = jnp.arange(NX, dtype=jnp.float32) / NX
    y_frac = jnp.arange(NY, dtype=jnp.float32) / NY
    z_frac = jnp.arange(NZ, dtype=jnp.float32) / NZ
    angles = 2.0 * jnp.pi * (winding[0] * x_frac[:, None, None, None] + winding[1] * y_frac[None, :, None, None] + winding[2] * z_frac[None, None, :, None])
    angles = angles + jax.random.uniform(subkeys[4], (NX, NY, NZ, NB), jnp.float32, -jitter, jitter)
    cosine = jnp.cos(angles)[..., None]
    sine = jnp.sin(angles)[..., None]
    real_part = cosine * fields[0] - sine * fields[1]
    imag_part = sine * fields[0] + cosine * fields[1]
    return jnp.stack([real_part, imag_part]).astype(jnp.bfloat16)


def setup_inputs(seed: int = 0) -> dict:
    arg_keys = jax.random.split(jax.random.key(seed), 3)
    coefficients = draw_coefficients(jax.random.fold_in(arg_keys[2], 71), 0)
    shift_blocks = draw_shift_blocks(jax.random.fold_in(arg_keys[2], 71), 0)
    return dict(coefficients=coefficients, shift_blocks=shift_blocks)


def pair_measure(own_point, partner):
    bands = own_point.shape[1]
    left_side = jnp.concatenate([own_point[0], own_point[1]], axis=1)
    right_side = jnp.concatenate([jnp.concatenate([partner[0], partner[1]], axis=1), jnp.concatenate([partner[1], -partner[0]], axis=1)], axis=0)
    product = jnp.dot(left_side, right_side.T, preferred_element_type=jnp.float32)
    real_part = product[:, :bands]
    imag_part = product[:, bands:]
    phases = jnp.arctan2(jnp.diagonal(imag_part), jnp.diagonal(real_part))
    coherence = jnp.sum(real_part * real_part + imag_part * imag_part) / bands
    return phases, coherence


def reference(coefficients, shift_blocks):
    shifts = shift_blocks.astype(jnp.int32) * 128
    k_total = NX * NY * NZ
    counts = jnp.array([NX, NY, NZ], jnp.float32)

    def per_point(k_index):
        x_index = k_index // (NY * NZ)
        y_index = (k_index // NZ) % NY
        z_index = k_index % NZ
        own_point = coefficients[:, x_index, y_index, z_index]
        gathered_phases = []
        gathered_coherence = []
        for direction in range(3):
            coords = [x_index, y_index, z_index]
            limits = [NX, NY, NZ]
            wrapped = coords[direction] == limits[direction] - 1
            coords[direction] = (coords[direction] + 1) % limits[direction]
            partner = coefficients[:, coords[0], coords[1], coords[2]]
            partner = jnp.where(wrapped, jnp.roll(partner, -shifts[direction], axis=-1), partner)
            phases, coherence = pair_measure(own_point, partner)
            gathered_phases.append(phases)
            gathered_coherence.append(coherence)
        return jnp.stack(gathered_phases), jnp.stack(gathered_coherence)

    phases, coherence = lax.map(per_point, jnp.arange(k_total, dtype=jnp.int32))
    mean_phase = jnp.sum(phases, axis=0) / k_total
    deviation = phases - mean_phase[None]
    variance = jnp.sum(deviation * deviation, axis=0) / k_total
    centre = -counts[:, None] * mean_phase / (2.0 * jnp.pi)
    spread = (counts[:, None] / (2.0 * jnp.pi)) ** 2 * variance
    coherence_out = coherence.T.reshape(3, NX, NY, NZ)
    return centre, spread, coherence_out
```

```python
import functools

import jax
import jax.numpy as jnp
from jax import lax
from jax.experimental import pallas as pl
from jax.experimental.pallas import tpu as pltpu
from jax.sharding import PartitionSpec as P

MESH = pl.DeviceIdType.MESH
AXES = ("kx", "ky", "kz")
LANES = 128
ROWS = 256
STRIP = 32


def greeted(count):
    return range(1, count) if count > 4 else sorted({1, count - 1})


def merged(parts, count):
    mean = functools.reduce(jnp.add, [part[0] for part in parts]) / len(parts)
    square = functools.reduce(jnp.add, [part[1] for part in parts])
    apart = functools.reduce(jnp.add, [(part[0] - mean) * (part[0] - mean) for part in parts])
    return mean, square + count * apart


def kernel(sizes, shift_ref, a_ref, sums_ref,
           own, partner, rolled, diag_re, diag_im, total, stats, heard,
           own_sem, send_sem, recv_sem, stat_send, stat_recv):
    planes, bands, width = own.shape[1:]
    chunks, cut = partner.shape[1], partner.shape[3]
    tiles, row_tiles = width // LANES, bands // ROWS
    place = [lax.axis_index(axis) for axis in AXES]
    points = [(d, p) for d in range(3) for p in range(planes)]

    def beside(d, step):
        return {AXES[d]: lax.rem(place[d] + step, sizes[d])}

    load = pltpu.make_async_copy(a_ref, own, own_sem)
    load.start()
    barrier = pltpu.get_barrier_semaphore()
    greetings = 0
    for d in range(3):
        for step in greeted(sizes[d]):
            pl.semaphore_signal(barrier, inc=1, device_id=beside(d, step), device_id_type=MESH)
            greetings += 1
    pl.semaphore_wait(barrier, greetings)

    def copy_of(i, c):
        d, p = points[i]
        source = (p + 1) % planes if d == 0 else p
        return pltpu.make_async_remote_copy(
            src_ref=a_ref.at[:, source, pl.ds(pl.multiple_of(c * cut, cut), cut), :],
            dst_ref=partner.at[i, c],
            send_sem=send_sem.at[i, c],
            recv_sem=recv_sem.at[i, c],
            device_id=beside(d, sizes[d] - 1),
            device_id_type=MESH,
        )

    def inner_copy(i, c):
        p = points[i][1]
        return pltpu.make_async_copy(
            a_ref.at[:, p + 1, pl.ds(pl.multiple_of(c * cut, cut), cut), :], partner.at[i, c], recv_sem.at[i, c]
        )

    def inner(i):
        d, p = points[i]
        return d == 0 and p < planes - 1

    def launch(c, carry):
        for i in range(len(points)):
            (inner_copy(i, c) if inner(i) else copy_of(i, c)).start()
        return carry

    lax.fori_loop(0, chunks, launch, 0)

    total[...] = jnp.zeros_like(total)
    diag_re[...] = jnp.zeros_like(diag_re)
    diag_im[...] = jnp.zeros_like(diag_im)
    load.wait()
    for i, (d, p) in enumerate(points):
        wraps = place[d] == sizes[d] - 1
        shift = 0 if inner(i) else jnp.where(wraps, shift_ref[d], 0)

        moves = [] if inner(i) else [(LANES << bit, (shift >> bit) & 1 == 1) for bit in range((tiles - 1).bit_length())]

        def turn(block, carry, i=i, p=p, moves=moves):
            rows = pl.ds(pl.multiple_of(block * STRIP, STRIP), STRIP)
            for part in range(2):
                value = own[part, p, rows, :]
                for amount, taken in moves:
                    moved = jnp.concatenate([value[:, width - amount:], value[:, :width - amount]], axis=1)
                    value = jnp.where(taken, moved, value)
                rolled[i, part, rows, :] = value
            return carry

        lax.fori_loop(0, bands // STRIP, turn, 0)

    row = lax.broadcasted_iota(jnp.int32, (ROWS, cut), 0)
    column = lax.broadcasted_iota(jnp.int32, (ROWS, cut), 1)

    def arrived(i, c):
        (inner_copy(i, c).wait if inner(i) else copy_of(i, c).wait_recv)()

    def measure(i, c, start, rows):
        left = rolled[i, :, pl.ds(pl.multiple_of(start, rows), rows), :].reshape(2 * rows, width)
        right = partner[i, c].reshape(2 * cut, width)
        product = lax.dot_general(left, right, (((1,), (1,)), ((), ())), preferred_element_type=jnp.float32)
        re = product[:rows, :cut] + product[rows:, cut:]
        im = product[:rows, cut:] - product[rows:, :cut]
        squares = re * re + im * im
        total[i] += jnp.sum(squares.reshape(rows // 8, 8, cut), axis=0)
        same = row[:rows] + start == column[:rows] + c * cut
        diag_re[i, pl.ds(c, 1), :] += jnp.sum(jnp.where(same, re, 0.0), axis=0, keepdims=True)
        diag_im[i, pl.ds(c, 1), :] += jnp.sum(jnp.where(same, im, 0.0), axis=0, keepdims=True)

    def whole(i, c):
        def one(r, carry):
            measure(i, c, r * ROWS, ROWS)
            return carry
        lax.fori_loop(0, row_tiles, one, 0)

    order = [i for d in (1, 0, 2) for i, point in enumerate(points) if point[0] == d]

    def chunk(c, carry):
        for i in order:
            arrived(i, c)
            whole(i, c)
        return carry

    lax.fori_loop(0, chunks - 1, chunk, 0)
    last = chunks - 1
    edge = bands - cut
    for i in order:
        arrived(i, last)
        if points[i][0] == 1:
            whole(i, last)
        else:
            measure(i, last, edge, cut)
    phases = jnp.arctan2(diag_im[...], diag_re[...])
    groups = phases.reshape(3, planes, chunks, cut)
    mean, square = merged([(groups[:, p], jnp.zeros_like(groups[:, p])) for p in range(planes)], 1.0)
    count = float(planes)

    def stat_copy(d, step):
        return pltpu.make_async_remote_copy(
            src_ref=stats.at[d],
            dst_ref=heard[d].at[step - 1],
            send_sem=stat_send[d].at[step - 1],
            recv_sem=stat_recv[d].at[step - 1],
            device_id=beside(d, step),
            device_id_type=MESH,
        )

    for d in range(3):
        stats[d, 0] = mean
        stats[d, 1] = square
        for step in range(1, sizes[d]):
            stat_copy(d, step).start()
        if d == 0:
            for i in order:
                if points[i][0] != 1:
                    for start in range(0, edge, ROWS):
                        measure(i, last, start, min(ROWS, edge - start))
        for step in range(1, sizes[d]):
            stat_copy(d, step).wait_recv()
        members = [(mean, square)] + [(heard[d][step - 1, 0], heard[d][step - 1, 1]) for step in range(1, sizes[d])]
        ordered = []
        for slot in range(sizes[d]):
            entry = None
            for step in range(sizes[d]):
                owner = lax.rem(place[d] - step + sizes[d], sizes[d])
                if entry is None:
                    entry = members[step]
                else:
                    entry = tuple(jnp.where(owner == slot, new, old) for new, old in zip(members[step], entry))
            ordered.append(entry)
        mean, square = merged(ordered, count)
        count *= sizes[d]

    for d in range(3):
        sums_ref[d * chunks:(d + 1) * chunks, :] = mean[d]
        sums_ref[(3 + d) * chunks:(4 + d) * chunks, :] = square[d]
    for i in range(len(points)):
        sums_ref[6 * chunks + 8 * i:6 * chunks + 8 * (i + 1), :] = total[i]

    for d in range(3):
        for step in range(1, sizes[d]):
            stat_copy(d, step).wait_send()

    def sent(c, carry):
        for i in range(len(points)):
            if not inner(i):
                copy_of(i, c).wait_send()
        return carry

    lax.fori_loop(0, chunks, sent, 0)


def results(sizes, planes, sums_ref, centre_ref, spread_ref, coherence_ref):
    bands = centre_ref.shape[1]
    chunks, count = bands // LANES, planes * sizes[0] * sizes[1] * sizes[2]
    lengths = (planes * sizes[0], sizes[1], sizes[2])
    for d in range(3):
        scale = lengths[d] / (2.0 * jnp.pi)
        for c in range(chunks):
            lanes = slice(c * LANES, (c + 1) * LANES)
            centre_ref[d:d + 1, lanes] = -scale * sums_ref[d * chunks + c:d * chunks + c + 1, :]
            at = (3 + d) * chunks + c
            spread_ref[d:d + 1, lanes] = scale * scale * (sums_ref[at:at + 1, :] / count)
    for i in range(3 * planes):
        at = 6 * chunks + 8 * i
        coherence_ref[i] = jnp.sum(sums_ref[at:at + 8, :]) / bands


def solution(mesh):
    sizes = tuple(mesh.shape[axis] for axis in AXES)

    def shards(coefficients, shift_blocks):
        planes, bands, width = coefficients.shape[1], coefficients.shape[4], coefficients.shape[5]
        own_planes = coefficients.reshape(2, planes, bands, width)
        chunks = bands // LANES
        pairs = 3 * planes
        vmem = pl.BlockSpec(memory_space=pltpu.VMEM)
        sums = pl.pallas_call(
            functools.partial(kernel, sizes),
            out_shape=pltpu.VMEM((6 * chunks + 8 * pairs, LANES), jnp.float32),
            in_specs=[pl.BlockSpec(memory_space=pltpu.SMEM), pl.BlockSpec(memory_space=pl.ANY)],
            out_specs=vmem,
            scratch_shapes=[
                pltpu.VMEM((2, planes, bands, width), jnp.bfloat16),
                pltpu.VMEM((pairs, chunks, 2, LANES, width), jnp.bfloat16),
                pltpu.VMEM((pairs, 2, bands, width), jnp.bfloat16),
                pltpu.VMEM((pairs, chunks, LANES), jnp.float32),
                pltpu.VMEM((pairs, chunks, LANES), jnp.float32),
                pltpu.VMEM((pairs, 8, LANES), jnp.float32),
                pltpu.VMEM((3, 2, 3, chunks, LANES), jnp.float32),
                [pltpu.VMEM((size - 1, 2, 3, chunks, LANES), jnp.float32) for size in sizes],
                pltpu.SemaphoreType.DMA,
                pltpu.SemaphoreType.DMA((pairs, chunks)),
                pltpu.SemaphoreType.DMA((pairs, chunks)),
                [pltpu.SemaphoreType.DMA((size - 1,)) for size in sizes],
                [pltpu.SemaphoreType.DMA((size - 1,)) for size in sizes],
            ],
            compiler_params=pltpu.CompilerParams(
                collective_id=0, has_side_effects=True, vmem_limit_bytes=60 * 1024 * 1024
            ),
        )(shift_blocks, own_planes)
        sums = pltpu.with_memory_space_constraint(sums, pltpu.VMEM)
        centre, spread, coherence = pl.pallas_call(
            functools.partial(results, sizes, planes),
            out_shape=(
                jax.ShapeDtypeStruct((3, bands), jnp.float32),
                jax.ShapeDtypeStruct((3, bands), jnp.float32),
                jax.ShapeDtypeStruct((pairs,), jnp.float32),
            ),
            in_specs=[vmem],
            out_specs=(vmem, vmem, pl.BlockSpec(memory_space=pltpu.SMEM)),
        )(sums)
        return centre, spread, coherence.reshape(3, planes, 1, 1)

    in_specs = (P(None, "kx", "ky", "kz", None, None), P())
    out_specs = (P(), P(), P(None, "kx", "ky", "kz"))
    return jax.shard_map(shards, mesh=mesh, in_specs=in_specs, out_specs=out_specs, check_vma=False)
```

```python
import functools

import jax
import jax.numpy as jnp
from jax import lax
from jax.experimental import pallas as pl
from jax.experimental.pallas import tpu as pltpu
from jax.sharding import PartitionSpec as P

MESH = pl.DeviceIdType.MESH
AXES = ("kx", "ky", "kz")
LANES = 128
ROWS = 256
STRIP = 32


def added(parts):
    return functools.reduce(jnp.add, parts)


class Plan:
    def __init__(self, sizes, bands, width):
        self.sizes = sizes
        self.bands, self.width = bands, width
        self.paired = sizes[0] == 2
        self.chunks = bands // LANES
        self.rows = 3 * self.chunks
        self.plane = sizes[0] * sizes[1]
        self.share = -(-self.rows // self.plane)
        self.workers = -(-(self.rows - 1) // self.share)
        self.devices = self.plane * sizes[2]
        self.slots = 4 if self.paired else 3
        self.rounds = [size // 2 for size in sizes]


def kernel(plan, shift_hbm, a_ref, sums_ref,
           shift_ref, own, partner, rolled, diag_re, diag_im, total,
           xres, xout, rows, pooled, levels, final, every,
           shift_sem, own_sem, send_sem, recv_sem, xres_sem,
           pool_send, pool_recv, level_send, level_recv, final_send, final_recv,
           every_send, every_recv, token):
    sizes, bands, width = plan.sizes, plan.bands, plan.width
    chunks, cut = plan.chunks, LANES
    tiles, row_tiles = width // LANES, bands // ROWS
    place = [lax.axis_index(axis) for axis in AXES]
    me_plane = place[0] * sizes[1] + place[1]
    me = me_plane * sizes[2] + place[2]

    def beside(d, step):
        return {AXES[d]: lax.rem(place[d] + step, sizes[d])}

    load = pltpu.make_async_copy(a_ref, own, own_sem)
    load.start()
    shifts = pltpu.make_async_copy(shift_hbm, shift_ref, shift_sem)
    shifts.start()

    barrier = pltpu.get_barrier_semaphore()
    greetings = 0
    for d in (2, 0, 1):
        for step in sorted({1, sizes[d] - 1}):
            pl.semaphore_signal(barrier, inc=1, device_id=beside(d, step), device_id_type=MESH)
            greetings += 1
    pl.semaphore_wait(barrier, greetings)

    def copy_of(d, c):
        return pltpu.make_async_remote_copy(
            src_ref=a_ref.at[:, pl.ds(pl.multiple_of(c * cut, cut), cut), :],
            dst_ref=partner.at[d, c],
            send_sem=send_sem.at[d, c],
            recv_sem=recv_sem.at[d, c],
            device_id=beside(d, sizes[d] - 1),
            device_id_type=MESH,
        )

    if plan.paired:
        computes = lax.rem(place[0] + place[1], 2) == 0
        yields = jnp.logical_not(computes)
    else:
        computes = yields = None

    def when(condition, act):
        if condition is None:
            act()
        else:
            pl.when(condition)(act)

    for c in range(chunks):
        copy_of(2, c).start()
    for c in range(chunks):
        when(yields, lambda: copy_of(0, c).start())
        copy_of(1, c).start()

    total[...] = jnp.zeros_like(total)
    diag_re[...] = jnp.zeros_like(diag_re)
    diag_im[...] = jnp.zeros_like(diag_im)
    rows[...] = jnp.zeros_like(rows)
    shifts.wait()
    load.wait()
    for d in range(3):
        if d == 0 and plan.paired:
            shift = jnp.where(place[d] == 0, tiles - shift_ref[d], shift_ref[d])
        else:
            shift = jnp.where(place[d] == sizes[d] - 1, shift_ref[d], 0)
        moves = [(LANES << bit, (shift >> bit) & 1 == 1) for bit in range((tiles - 1).bit_length())]

        def turn(block, carry, d=d, moves=moves):
            strip = pl.ds(pl.multiple_of(block * STRIP, STRIP), STRIP)
            for part in range(2):
                value = own[part, strip, :]
                for amount, taken in moves:
                    moved = jnp.concatenate([value[:, width - amount:], value[:, :width - amount]], axis=1)
                    value = jnp.where(taken, moved, value)
                rolled[d, part, strip, :] = value
            return carry

        lax.fori_loop(0, bands // STRIP, turn, 0)

    for d in (1, 0, 2):
        steps = sorted({1, sizes[d] - 1})
        for turn_no in range(plan.rounds[d]):
            for way, step in enumerate(steps):
                pl.semaphore_signal(
                    token[d].at[turn_no, way], inc=1, device_id=beside(d, step), device_id_type=MESH
                )
            for way in range(len(steps)):
                pl.semaphore_wait(token[d].at[turn_no, way], 1)

    row = lax.broadcasted_iota(jnp.int32, (ROWS, cut), 0)
    column = lax.broadcasted_iota(jnp.int32, (ROWS, cut), 1)

    def measure(slot, left_ref, d, c, start, count):
        left = left_ref[:, pl.ds(pl.multiple_of(start, count), count), :].reshape(2 * count, width)
        right = partner[d, c].reshape(2 * cut, width)
        product = lax.dot_general(left, right, (((1,), (1,)), ((), ())), preferred_element_type=jnp.float32)
        re = product[:count, :cut] + product[count:, cut:]
        im = product[:count, cut:] - product[count:, :cut]
        squares = re * re + im * im
        total[slot] += jnp.sum(squares.reshape(count // 8, 8, cut), axis=0)
        same = row[:count] + start == column[:count] + c * cut
        diag_re[slot, pl.ds(c, 1), :] += jnp.sum(jnp.where(same, re, 0.0), axis=0, keepdims=True)
        diag_im[slot, pl.ds(c, 1), :] += jnp.sum(jnp.where(same, im, 0.0), axis=0, keepdims=True)

    def whole(slot, left_ref, d, c):
        def one(r, carry):
            measure(slot, left_ref, d, c, r * ROWS, ROWS)
            return carry
        lax.fori_loop(0, row_tiles, one, 0)

    y_slot, z_slot = plan.slots - 2, plan.slots - 1

    def chunk(c, carry):
        copy_of(1, c).wait_recv()
        whole(y_slot, rolled.at[1], 1, c)

        def along_x():
            copy_of(0, c).wait_recv()
            if plan.paired:
                whole(0, own, 0, c)
                whole(1, rolled.at[0], 0, c)
            else:
                whole(0, rolled.at[0], 0, c)

        when(computes, along_x)
        return carry

    lax.fori_loop(0, chunks, chunk, 0)

    def phases(slot, sign=None):
        im = diag_im[slot] if sign is None else sign * diag_im[slot]
        return jnp.arctan2(im, diag_re[slot])

    xres_copy = pltpu.make_async_remote_copy(
        src_ref=xout, dst_ref=xres, send_sem=xres_sem.at[0], recv_sem=xres_sem.at[1],
        device_id=beside(0, sizes[0] - 1), device_id_type=MESH,
    )
    if plan.paired:
        def share_x():
            first = place[0] == 0
            sign = jnp.where(first, 1.0, -1.0)
            low, high = phases(0, sign), phases(1, -sign)
            xres[:chunks] = jnp.where(first, low, high)
            xres[chunks:] = jnp.where(first, total[0], total[1])
            xout[:chunks] = jnp.where(first, high, low)
            xout[chunks:] = jnp.where(first, total[1], total[0])
            xres_copy.start()

        pl.when(computes)(share_x)
    else:
        xres[:chunks] = phases(0)
        xres[chunks:] = total[0]

    def along_z(c, carry):
        copy_of(2, c).wait_recv()
        whole(z_slot, rolled.at[2], 2, c)
        return carry

    last = chunks - 1
    lax.fori_loop(0, last, along_z, 0)

    if plan.paired:
        pl.when(yields)(lambda: xres_copy.wait_recv())
    found = [xres[:chunks], phases(y_slot), phases(z_slot)]
    for d in range(3):
        for c in range(chunks):
            if d * chunks + c < plan.rows - 1:
                rows[d * chunks + c] = found[d][c:c + 1]

    share, workers, plane = plan.share, plan.workers, plan.plane
    mine = pl.ds(me_plane * share, share)
    works = me_plane < workers

    def spot(p):
        return {"kx": p // sizes[1], "ky": p % sizes[1]}

    def pool_copy(source, worker):
        return pltpu.make_async_remote_copy(
            src_ref=rows.at[pl.ds(worker * share, share)], dst_ref=pooled.at[source],
            send_sem=pool_send.at[worker], recv_sem=pool_recv.at[source],
            device_id=spot(worker), device_id_type=MESH,
        )

    for worker in range(workers):
        pl.when(me_plane != worker)(lambda worker=worker: pool_copy(me_plane, worker).start())

    def level_copy(step):
        return pltpu.make_async_remote_copy(
            src_ref=levels.at[0], dst_ref=levels.at[step],
            send_sem=level_send.at[step], recv_sem=level_recv.at[step],
            device_id=beside(2, step), device_id_type=MESH,
        )

    def final_copy(worker, p):
        return pltpu.make_async_remote_copy(
            src_ref=final.at[pl.ds(worker * share, share)], dst_ref=final.at[pl.ds(worker * share, share)],
            send_sem=final_send.at[p], recv_sem=final_recv.at[worker],
            device_id=spot(p), device_id_type=MESH,
        )

    def pool():
        pooled[me_plane] = rows[mine]
        for p in range(plane):
            pl.when(me_plane != p)(lambda p=p: pool_copy(p, 0).wait_recv())
        mean = added([pooled[p] for p in range(plane)]) / plane
        square = added([(pooled[p] - mean) * (pooled[p] - mean) for p in range(plane)])
        levels[0, 0] = mean
        levels[0, 1] = square
        for step in range(1, sizes[2]):
            level_copy(step).start()

    def merge():
        for step in range(1, sizes[2]):
            level_copy(step).wait_recv()
        heard = []
        for z in range(sizes[2]):
            at = lax.rem(place[2] - z + sizes[2], sizes[2])
            heard.append((levels[at, 0], levels[at, 1]))
        mean = added([part[0] for part in heard]) / sizes[2]
        square = added([part[1] for part in heard])
        apart = added([(part[0] - mean) * (part[0] - mean) for part in heard])
        square = square + plane * apart
        for w in range(share):
            final[me_plane * share + w, 0] = mean[w]
            final[me_plane * share + w, 1] = square[w]
        for p in range(plane):
            pl.when(me_plane != p)(lambda p=p: final_copy(me_plane, p).start())

    pl.when(works)(pool)
    pl.when(works)(merge)
    for worker in range(workers):
        pl.when(me_plane != worker)(lambda worker=worker: final_copy(worker, 0).wait_recv())

    edge = bands - cut
    copy_of(2, last).wait_recv()
    measure(z_slot, rolled.at[2], 2, last, edge, cut)
    every[me] = jnp.arctan2(diag_im[z_slot, last:last + 1], diag_re[z_slot, last:last + 1])

    def every_copy(slot, x, y, z):
        return pltpu.make_async_remote_copy(
            src_ref=every.at[me], dst_ref=every.at[me],
            send_sem=every_send.at[slot], recv_sem=every_recv.at[me],
            device_id={"kx": x, "ky": y, "kz": z}, device_id_type=MESH,
        )

    def heard_from(other):
        return pltpu.make_async_remote_copy(
            src_ref=every.at[me], dst_ref=every.at[other],
            send_sem=every_send.at[0], recv_sem=every_recv.at[other],
            device_id=beside(2, 1), device_id_type=MESH,
        )

    def place_of(slot):
        return slot // (sizes[1] * sizes[2]), (slot // sizes[2]) % sizes[1], slot % sizes[2]

    def each(act):
        if plan.devices <= 64:
            for slot in range(1, plan.devices):
                act(slot)
        else:
            def one(slot, carry):
                act(slot)
                return carry
            lax.fori_loop(1, plan.devices, one, 0)

    def offset(slot):
        return [lax.rem(place[d] + step, sizes[d]) for d, step in enumerate(place_of(slot))]

    each(lambda slot: every_copy(slot, *offset(slot)).start())
    for start in range(0, edge, ROWS):
        measure(z_slot, rolled.at[2], 2, last, start, min(ROWS, edge - start))

    totals = [xres[chunks:], total[y_slot], total[z_slot]]
    for d in range(3):
        sums_ref[2 * plan.rows + 8 * d:2 * plan.rows + 8 * (d + 1), :] = totals[d]
    for r in range(plan.rows - 1):
        sums_ref[r:r + 1, :] = final[r, 0]
        sums_ref[plan.rows + r:plan.rows + r + 1, :] = final[r, 1]

    def hear(slot):
        x, y, z = offset(slot)
        heard_from((x * sizes[1] + y) * sizes[2] + z).wait_recv()

    each(hear)
    if plan.devices <= 64:
        mean = added([every[k] for k in range(plan.devices)]) / plan.devices
        square = added([(every[k] - mean) * (every[k] - mean) for k in range(plan.devices)])
    else:
        zero = jnp.zeros((1, cut), jnp.float32)
        mean = lax.fori_loop(0, plan.devices, lambda k, sofar: sofar + every[k], zero) / plan.devices
        square = lax.fori_loop(
            0, plan.devices, lambda k, sofar: sofar + (every[k] - mean) * (every[k] - mean), zero
        )
    sums_ref[plan.rows - 1:plan.rows, :] = mean
    sums_ref[2 * plan.rows - 1:2 * plan.rows, :] = square

    each(lambda slot: every_copy(slot, *offset(slot)).wait_send())
    for worker in range(workers):
        pl.when(me_plane != worker)(lambda worker=worker: pool_copy(me_plane, worker).wait_send())

    def settle():
        for step in range(1, sizes[2]):
            level_copy(step).wait_send()
        for p in range(plane):
            pl.when(me_plane != p)(lambda p=p: final_copy(me_plane, p).wait_send())

    pl.when(works)(settle)
    if plan.paired:
        pl.when(computes)(lambda: xres_copy.wait_send())

    for c in range(chunks):
        when(yields, lambda: copy_of(0, c).wait_send())
        copy_of(1, c).wait_send()
        copy_of(2, c).wait_send()


def results(plan, sums_ref, centre_ref, spread_ref, coherence_ref):
    chunks, count = plan.chunks, plan.devices
    for d in range(3):
        scale = plan.sizes[d] / (2.0 * jnp.pi)
        for c in range(chunks):
            lanes = slice(c * LANES, (c + 1) * LANES)
            at = d * chunks + c
            centre_ref[d:d + 1, lanes] = -scale * sums_ref[at:at + 1, :]
            at += plan.rows
            spread_ref[d:d + 1, lanes] = scale * scale * (sums_ref[at:at + 1, :] / count)
    for d in range(3):
        at = 2 * plan.rows + 8 * d
        coherence_ref[d] = jnp.sum(sums_ref[at:at + 8, :]) / plan.bands


def solution(mesh):
    sizes = tuple(mesh.shape[axis] for axis in AXES)

    def shards(coefficients, shift_blocks):
        bands, width = coefficients.shape[4], coefficients.shape[5]
        plan = Plan(sizes, bands, width)
        chunks = plan.chunks
        vmem = pl.BlockSpec(memory_space=pltpu.VMEM)
        hbm = pl.BlockSpec(memory_space=pl.ANY)
        dma = pltpu.SemaphoreType.DMA
        padded = plan.plane * plan.share
        sums = pl.pallas_call(
            functools.partial(kernel, plan),
            out_shape=pltpu.VMEM((2 * plan.rows + 24, LANES), jnp.float32),
            in_specs=[hbm, hbm],
            out_specs=vmem,
            scratch_shapes=[
                pltpu.SMEM((3,), jnp.int32),
                pltpu.VMEM((2, bands, width), jnp.bfloat16),
                pltpu.VMEM((3, chunks, 2, LANES, width), jnp.bfloat16),
                pltpu.VMEM((3, 2, bands, width), jnp.bfloat16),
                pltpu.VMEM((plan.slots, chunks, LANES), jnp.float32),
                pltpu.VMEM((plan.slots, chunks, LANES), jnp.float32),
                pltpu.VMEM((plan.slots, 8, LANES), jnp.float32),
                pltpu.VMEM((chunks + 8, LANES), jnp.float32),
                pltpu.VMEM((chunks + 8, LANES), jnp.float32),
                pltpu.VMEM((padded, 1, LANES), jnp.float32),
                pltpu.VMEM((plan.plane, plan.share, 1, LANES), jnp.float32),
                pltpu.VMEM((sizes[2], 2, plan.share, 1, LANES), jnp.float32),
                pltpu.VMEM((padded, 2, 1, LANES), jnp.float32),
                pltpu.VMEM((plan.devices, 1, LANES), jnp.float32),
                dma,
                dma,
                dma((3, chunks)),
                dma((3, chunks)),
                dma((2,)),
                dma((plan.workers,)),
                dma((plan.plane,)),
                dma((sizes[2],)),
                dma((sizes[2],)),
                dma((plan.plane,)),
                dma((plan.workers,)),
                dma((plan.devices,)),
                dma((plan.devices,)),
                [pltpu.SemaphoreType.REGULAR((rounds, 2)) for rounds in plan.rounds],
            ],
            compiler_params=pltpu.CompilerParams(
                collective_id=0, has_side_effects=True, vmem_limit_bytes=60 * 1024 * 1024
            ),
        )(shift_blocks, coefficients.reshape(2, bands, width))
        sums = pltpu.with_memory_space_constraint(sums, pltpu.VMEM)
        centre, spread, coherence = pl.pallas_call(
            functools.partial(results, plan),
            out_shape=(
                jax.ShapeDtypeStruct((3, bands), jnp.float32),
                jax.ShapeDtypeStruct((3, bands), jnp.float32),
                jax.ShapeDtypeStruct((3,), jnp.float32),
            ),
            in_specs=[vmem],
            out_specs=(vmem, vmem, pl.BlockSpec(memory_space=pltpu.SMEM)),
        )(sums)
        return centre, spread, coherence.reshape(3, 1, 1, 1)

    in_specs = (P(None, "kx", "ky", "kz", None, None), P())
    out_specs = (P(), P(), P(None, "kx", "ky", "kz"))
    return jax.shard_map(shards, mesh=mesh, in_specs=in_specs, out_specs=out_specs, check_vma=False)
```

```python
import functools

import jax
import jax.numpy as jnp
from jax import lax
from jax.experimental import pallas as pl
from jax.experimental.pallas import tpu as pltpu
from jax.sharding import PartitionSpec as P

MESH = pl.DeviceIdType.MESH
AXES = ("kx", "ky", "kz")
LANES = 128
ROWS = 256
STRIP = 32


def added(parts):
    return functools.reduce(jnp.add, parts)


class Plan:
    def __init__(self, sizes, bands, width):
        self.sizes = sizes
        self.bands, self.width = bands, width
        self.paired = sizes[0] == 2
        self.chunks = bands // LANES
        self.rows = 3 * self.chunks
        self.plane = sizes[0] * sizes[1]
        self.share = -(-self.rows // self.plane)
        self.workers = -(-(self.rows - 1) // self.share)
        self.devices = self.plane * sizes[2]
        self.slots = 4 if self.paired else 3
        self.toward = [sizes[0] - 1, sizes[1] - 1, 1]
        self.half = LANES // 2


def kernel(plan, shift_hbm, a_ref, sums_ref,
           shift_ref, own, partner, rolled, diag_re, diag_im, total,
           xres, xout, ztotal, rows, pooled, levels, final, every,
           shift_sem, own_sem, send_sem, recv_sem, xres_sem,
           pool_send, pool_recv, level_send, level_recv, final_send, final_recv,
           every_send, every_recv, token):
    sizes, bands, width = plan.sizes, plan.bands, plan.width
    chunks, cut = plan.chunks, LANES
    tiles, row_tiles = width // LANES, bands // ROWS
    place = [lax.axis_index(axis) for axis in AXES]
    me_plane = place[0] * sizes[1] + place[1]
    me = me_plane * sizes[2] + place[2]

    def beside(d, step):
        return {AXES[d]: lax.rem(place[d] + step, sizes[d])}

    load = pltpu.make_async_copy(a_ref, own, own_sem)
    load.start()
    shifts = pltpu.make_async_copy(shift_hbm, shift_ref, shift_sem)
    shifts.start()

    barrier = pltpu.get_barrier_semaphore()
    for d in (2, 0, 1):
        source = beside(d, sizes[d] - plan.toward[d])
        pl.semaphore_signal(barrier, inc=1, device_id=source, device_id_type=MESH)
    pl.semaphore_wait(barrier, 3)

    def copy_of(d, c):
        return pltpu.make_async_remote_copy(
            src_ref=a_ref.at[:, pl.ds(pl.multiple_of(c * cut, cut), cut), :],
            dst_ref=partner.at[d, c],
            send_sem=send_sem.at[d, c],
            recv_sem=recv_sem.at[d, c],
            device_id=beside(d, plan.toward[d]),
            device_id_type=MESH,
        )

    last, half = chunks - 1, plan.half

    def tail_copy(part):
        return pltpu.make_async_remote_copy(
            src_ref=a_ref.at[:, pl.ds(last * cut + part * half, half), :],
            dst_ref=partner.at[2, last, :, pl.ds(part * half, half), :],
            send_sem=send_sem.at[2, last + part],
            recv_sem=recv_sem.at[2, last + part],
            device_id=beside(2, plan.toward[2]),
            device_id_type=MESH,
        )

    if plan.paired:
        computes = lax.rem(place[0] + place[1], 2) == 0
        yields = jnp.logical_not(computes)
    else:
        computes = yields = None

    def when(condition, act):
        if condition is None:
            act()
        else:
            pl.when(condition)(act)

    for c in range(last):
        copy_of(2, c).start()
    tail_copy(0).start()
    for c in range(chunks):
        when(yields, lambda: copy_of(0, c).start())
        copy_of(1, c).start()

    total[...] = jnp.zeros_like(total)
    diag_re[...] = jnp.zeros_like(diag_re)
    diag_im[...] = jnp.zeros_like(diag_im)
    rows[...] = jnp.zeros_like(rows)
    shifts.wait()
    load.wait()
    for d in range(3):
        if d == 0 and plan.paired:
            shift = jnp.where(place[d] == 0, tiles - shift_ref[d], shift_ref[d])
        elif d == 2:
            shift = jnp.where(place[d] == 0, tiles - shift_ref[d], 0)
        else:
            shift = jnp.where(place[d] == sizes[d] - 1, shift_ref[d], 0)
        moves = [(LANES << bit, (shift >> bit) & 1 == 1) for bit in range((tiles - 1).bit_length())]

        def turn(block, carry, d=d, moves=moves):
            strip = pl.ds(pl.multiple_of(block * STRIP, STRIP), STRIP)
            for part in range(2):
                value = own[part, strip, :]
                for amount, taken in moves:
                    moved = jnp.concatenate([value[:, width - amount:], value[:, :width - amount]], axis=1)
                    value = jnp.where(taken, moved, value)
                rolled[d, part, strip, :] = value
            return carry

        lax.fori_loop(0, bands // STRIP, turn, 0)

    for d in (1, 0, 2):
        for turn_no in range(sizes[d] - 1):
            pl.semaphore_signal(
                token[d].at[turn_no], inc=1, device_id=beside(d, plan.toward[d]), device_id_type=MESH
            )
            pl.semaphore_wait(token[d].at[turn_no], 1)

    row = lax.broadcasted_iota(jnp.int32, (ROWS, cut), 0)
    column = lax.broadcasted_iota(jnp.int32, (ROWS, cut), 1)

    def measure(slot, left_ref, d, c, start, count):
        left = left_ref[:, pl.ds(pl.multiple_of(start, count), count), :].reshape(2 * count, width)
        right = partner[d, c].reshape(2 * cut, width)
        product = lax.dot_general(left, right, (((1,), (1,)), ((), ())), preferred_element_type=jnp.float32)
        re = product[:count, :cut] + product[count:, cut:]
        im = product[:count, cut:] - product[count:, :cut]
        squares = re * re + im * im
        total[slot] += jnp.sum(squares.reshape(count // 8, 8, cut), axis=0)
        same = row[:count] + start == column[:count] + c * cut
        diag_re[slot, pl.ds(c, 1), :] += jnp.sum(jnp.where(same, re, 0.0), axis=0, keepdims=True)
        diag_im[slot, pl.ds(c, 1), :] += jnp.sum(jnp.where(same, im, 0.0), axis=0, keepdims=True)

    def whole(slot, left_ref, d, c):
        def one(r, carry):
            measure(slot, left_ref, d, c, r * ROWS, ROWS)
            return carry
        lax.fori_loop(0, row_tiles, one, 0)

    y_slot, z_slot = plan.slots - 2, plan.slots - 1

    def chunk(c, carry):
        copy_of(1, c).wait_recv()
        whole(y_slot, rolled.at[1], 1, c)

        def along_x():
            copy_of(0, c).wait_recv()
            if plan.paired:
                whole(0, own, 0, c)
                whole(1, rolled.at[0], 0, c)
            else:
                whole(0, rolled.at[0], 0, c)

        when(computes, along_x)
        return carry

    lax.fori_loop(0, chunks, chunk, 0)

    def phases(slot, sign=None):
        im = diag_im[slot] if sign is None else sign * diag_im[slot]
        return jnp.arctan2(im, diag_re[slot])

    xres_copy = pltpu.make_async_remote_copy(
        src_ref=xout, dst_ref=xres, send_sem=xres_sem.at[0], recv_sem=xres_sem.at[1],
        device_id=beside(0, sizes[0] - 1), device_id_type=MESH,
    )
    if plan.paired:
        def share_x():
            first = place[0] == 0
            sign = jnp.where(first, 1.0, -1.0)
            low, high = phases(0, sign), phases(1, -sign)
            xres[:chunks] = jnp.where(first, low, high)
            xres[chunks:] = jnp.where(first, total[0], total[1])
            xout[:chunks] = jnp.where(first, high, low)
            xout[chunks:] = jnp.where(first, total[1], total[0])
            xres_copy.start()

        pl.when(computes)(share_x)
    else:
        xres[:chunks] = phases(0)
        xres[chunks:] = total[0]

    def along_z(c, carry):
        copy_of(2, c).wait_recv()
        whole(z_slot, rolled.at[2], 2, c)
        return carry

    lax.fori_loop(0, last, along_z, 0)

    if plan.paired:
        pl.when(yields)(lambda: xres_copy.wait_recv())
    found = [xres[:chunks], phases(y_slot), phases(z_slot, -1.0)]
    for d in range(3):
        for c in range(chunks):
            if d * chunks + c < plan.rows - 1:
                rows[d * chunks + c] = found[d][c:c + 1]

    share, workers, plane = plan.share, plan.workers, plan.plane
    mine = pl.ds(me_plane * share, share)
    works = me_plane < workers

    def spot(p):
        return {"kx": p // sizes[1], "ky": p % sizes[1]}

    def pool_copy(source, worker):
        return pltpu.make_async_remote_copy(
            src_ref=rows.at[pl.ds(worker * share, share)], dst_ref=pooled.at[source],
            send_sem=pool_send.at[worker], recv_sem=pool_recv.at[source],
            device_id=spot(worker), device_id_type=MESH,
        )

    for worker in range(workers):
        pl.when(me_plane != worker)(lambda worker=worker: pool_copy(me_plane, worker).start())

    def level_copy(step):
        return pltpu.make_async_remote_copy(
            src_ref=levels.at[0], dst_ref=levels.at[step],
            send_sem=level_send.at[step], recv_sem=level_recv.at[step],
            device_id=beside(2, step), device_id_type=MESH,
        )

    def final_copy(worker, p):
        return pltpu.make_async_remote_copy(
            src_ref=final.at[pl.ds(worker * share, share)], dst_ref=final.at[pl.ds(worker * share, share)],
            send_sem=final_send.at[p], recv_sem=final_recv.at[worker],
            device_id=spot(p), device_id_type=MESH,
        )

    def pool():
        pooled[me_plane] = rows[mine]
        for p in range(plane):
            pl.when(me_plane != p)(lambda p=p: pool_copy(p, 0).wait_recv())
        mean = added([pooled[p] for p in range(plane)]) / plane
        square = added([(pooled[p] - mean) * (pooled[p] - mean) for p in range(plane)])
        levels[0, 0] = mean
        levels[0, 1] = square
        for step in range(1, sizes[2]):
            level_copy(step).start()

    def merge():
        for step in range(1, sizes[2]):
            level_copy(step).wait_recv()
        heard = []
        for z in range(sizes[2]):
            at = lax.rem(place[2] - z + sizes[2], sizes[2])
            heard.append((levels[at, 0], levels[at, 1]))
        mean = added([part[0] for part in heard]) / sizes[2]
        square = added([part[1] for part in heard])
        apart = added([(part[0] - mean) * (part[0] - mean) for part in heard])
        square = square + plane * apart
        for w in range(share):
            final[me_plane * share + w, 0] = mean[w]
            final[me_plane * share + w, 1] = square[w]
        for p in range(plane):
            pl.when(me_plane != p)(lambda p=p: final_copy(me_plane, p).start())

    pl.when(works)(pool)
    tail_copy(1).start()
    pl.when(works)(merge)
    for worker in range(workers):
        pl.when(me_plane != worker)(lambda worker=worker: final_copy(worker, 0).wait_recv())

    edge = bands - cut
    for part in range(2):
        tail_copy(part).wait_recv()
    measure(z_slot, rolled.at[2], 2, last, edge, cut)
    every[me] = jnp.arctan2(-diag_im[z_slot, last:last + 1], diag_re[z_slot, last:last + 1])

    def every_copy(slot, x, y, z):
        return pltpu.make_async_remote_copy(
            src_ref=every.at[me], dst_ref=every.at[me],
            send_sem=every_send.at[slot], recv_sem=every_recv.at[me],
            device_id={"kx": x, "ky": y, "kz": z}, device_id_type=MESH,
        )

    def heard_from(other):
        return pltpu.make_async_remote_copy(
            src_ref=every.at[me], dst_ref=every.at[other],
            send_sem=every_send.at[0], recv_sem=every_recv.at[other],
            device_id=beside(2, 1), device_id_type=MESH,
        )

    def place_of(slot):
        return slot // (sizes[1] * sizes[2]), (slot // sizes[2]) % sizes[1], slot % sizes[2]

    def each(act):
        if plan.devices <= 64:
            for slot in range(1, plan.devices):
                act(slot)
        else:
            def one(slot, carry):
                act(slot)
                return carry
            lax.fori_loop(1, plan.devices, one, 0)

    def offset(slot):
        return [lax.rem(place[d] + step, sizes[d]) for d, step in enumerate(place_of(slot))]

    each(lambda slot: every_copy(slot, *offset(slot)).start())
    for start in range(0, edge, ROWS):
        measure(z_slot, rolled.at[2], 2, last, start, min(ROWS, edge - start))

    ztotal_copy = pltpu.make_async_remote_copy(
        src_ref=total.at[z_slot], dst_ref=ztotal, send_sem=xres_sem.at[2], recv_sem=xres_sem.at[3],
        device_id=beside(2, sizes[2] - plan.toward[2]), device_id_type=MESH,
    )
    for r in range(plan.rows - 1):
        sums_ref[r:r + 1, :] = final[r, 0]
        sums_ref[plan.rows + r:plan.rows + r + 1, :] = final[r, 1]
    ztotal_copy.start()

    def hear(slot):
        x, y, z = offset(slot)
        heard_from((x * sizes[1] + y) * sizes[2] + z).wait_recv()

    each(hear)
    if plan.devices <= 64:
        mean = added([every[k] for k in range(plan.devices)]) / plan.devices
        square = added([(every[k] - mean) * (every[k] - mean) for k in range(plan.devices)])
    else:
        zero = jnp.zeros((1, cut), jnp.float32)
        mean = lax.fori_loop(0, plan.devices, lambda k, sofar: sofar + every[k], zero) / plan.devices
        square = lax.fori_loop(
            0, plan.devices, lambda k, sofar: sofar + (every[k] - mean) * (every[k] - mean), zero
        )
    ztotal_copy.wait_recv()
    totals = [xres[chunks:], total[y_slot], ztotal[...]]
    for d in range(3):
        sums_ref[2 * plan.rows + 8 * d:2 * plan.rows + 8 * (d + 1), :] = totals[d]
    sums_ref[plan.rows - 1:plan.rows, :] = mean
    sums_ref[2 * plan.rows - 1:2 * plan.rows, :] = square

    each(lambda slot: every_copy(slot, *offset(slot)).wait_send())
    for worker in range(workers):
        pl.when(me_plane != worker)(lambda worker=worker: pool_copy(me_plane, worker).wait_send())

    def settle():
        for step in range(1, sizes[2]):
            level_copy(step).wait_send()
        for p in range(plane):
            pl.when(me_plane != p)(lambda p=p: final_copy(me_plane, p).wait_send())

    pl.when(works)(settle)
    if plan.paired:
        pl.when(computes)(lambda: xres_copy.wait_send())

    for c in range(chunks):
        when(yields, lambda: copy_of(0, c).wait_send())
        copy_of(1, c).wait_send()
        if c < last:
            copy_of(2, c).wait_send()
    for part in range(2):
        tail_copy(part).wait_send()
    ztotal_copy.wait_send()


def results(plan, sums_ref, centre_ref, spread_ref, coherence_ref):
    chunks, count = plan.chunks, plan.devices
    for d in range(3):
        scale = plan.sizes[d] / (2.0 * jnp.pi)
        for c in range(chunks):
            lanes = slice(c * LANES, (c + 1) * LANES)
            at = d * chunks + c
            centre_ref[d:d + 1, lanes] = -scale * sums_ref[at:at + 1, :]
            at += plan.rows
            spread_ref[d:d + 1, lanes] = scale * scale * (sums_ref[at:at + 1, :] / count)
    for d in range(3):
        at = 2 * plan.rows + 8 * d
        coherence_ref[d] = jnp.sum(sums_ref[at:at + 8, :]) / plan.bands


def solution(mesh):
    sizes = tuple(mesh.shape[axis] for axis in AXES)

    def shards(coefficients, shift_blocks):
        bands, width = coefficients.shape[4], coefficients.shape[5]
        plan = Plan(sizes, bands, width)
        chunks = plan.chunks
        vmem = pl.BlockSpec(memory_space=pltpu.VMEM)
        hbm = pl.BlockSpec(memory_space=pl.ANY)
        dma = pltpu.SemaphoreType.DMA
        padded = plan.plane * plan.share
        sums = pl.pallas_call(
            functools.partial(kernel, plan),
            out_shape=pltpu.VMEM((2 * plan.rows + 24, LANES), jnp.float32),
            in_specs=[hbm, hbm],
            out_specs=vmem,
            scratch_shapes=[
                pltpu.SMEM((3,), jnp.int32),
                pltpu.VMEM((2, bands, width), jnp.bfloat16),
                pltpu.VMEM((3, chunks, 2, LANES, width), jnp.bfloat16),
                pltpu.VMEM((3, 2, bands, width), jnp.bfloat16),
                pltpu.VMEM((plan.slots, chunks, LANES), jnp.float32),
                pltpu.VMEM((plan.slots, chunks, LANES), jnp.float32),
                pltpu.VMEM((plan.slots, 8, LANES), jnp.float32),
                pltpu.VMEM((chunks + 8, LANES), jnp.float32),
                pltpu.VMEM((chunks + 8, LANES), jnp.float32),
                pltpu.VMEM((8, LANES), jnp.float32),
                pltpu.VMEM((padded, 1, LANES), jnp.float32),
                pltpu.VMEM((plan.plane, plan.share, 1, LANES), jnp.float32),
                pltpu.VMEM((sizes[2], 2, plan.share, 1, LANES), jnp.float32),
                pltpu.VMEM((padded, 2, 1, LANES), jnp.float32),
                pltpu.VMEM((plan.devices, 1, LANES), jnp.float32),
                dma,
                dma,
                dma((3, chunks + 1)),
                dma((3, chunks + 1)),
                dma((4,)),
                dma((plan.workers,)),
                dma((plan.plane,)),
                dma((sizes[2],)),
                dma((sizes[2],)),
                dma((plan.plane,)),
                dma((plan.workers,)),
                dma((plan.devices,)),
                dma((plan.devices,)),
                [pltpu.SemaphoreType.REGULAR((size - 1,)) for size in sizes],
            ],
            compiler_params=pltpu.CompilerParams(
                collective_id=0, has_side_effects=True, vmem_limit_bytes=60 * 1024 * 1024
            ),
        )(shift_blocks, coefficients.reshape(2, bands, width))
        sums = pltpu.with_memory_space_constraint(sums, pltpu.VMEM)
        centre, spread, coherence = pl.pallas_call(
            functools.partial(results, plan),
            out_shape=(
                jax.ShapeDtypeStruct((3, bands), jnp.float32),
                jax.ShapeDtypeStruct((3, bands), jnp.float32),
                jax.ShapeDtypeStruct((3,), jnp.float32),
            ),
            in_specs=[vmem],
            out_specs=(vmem, vmem, pl.BlockSpec(memory_space=pltpu.SMEM)),
        )(sums)
        return centre, spread, coherence.reshape(3, 1, 1, 1)

    in_specs = (P(None, "kx", "ky", "kz", None, None), P())
    out_specs = (P(), P(), P(None, "kx", "ky", "kz"))
    return jax.shard_map(shards, mesh=mesh, in_specs=in_specs, out_specs=out_specs, check_vma=False)
```

```python
import functools

import jax
import jax.numpy as jnp
from jax import lax
from jax.experimental import pallas as pl
from jax.experimental.pallas import tpu as pltpu
from jax.sharding import PartitionSpec as P

MESH = pl.DeviceIdType.MESH
AXES = ("kx", "ky", "kz")
LANES = 128
ROWS = 256
STRIP = 32


def added(parts):
    while len(parts) > 1:
        parts = [a + b for a, b in zip(parts[::2], parts[1::2])] + parts[len(parts) // 2 * 2:]
    return parts[0]


class Plan:
    def __init__(self, sizes, bands, width):
        self.sizes = sizes
        self.bands, self.width = bands, width
        self.paired = sizes[0] == 2
        self.chunks = bands // LANES
        self.rows = 3 * self.chunks
        self.plane = sizes[0] * sizes[1]
        self.share = -(-self.rows // self.plane)
        self.workers = -(-(self.rows - 1) // self.share)
        self.devices = self.plane * sizes[2]
        self.slots = 4 if self.paired else 3
        self.toward = [sizes[0] - 1, sizes[1] - 1, 1]
        self.parts = ((0, 64), (64, 32), (96, 32))


def kernel(plan, shift_hbm, a_ref, sums_ref,
           shift_ref, own, partner, rolled, diag_re, diag_im, total,
           xres, xout, ztotal, rows, pooled, levels, final, every,
           shift_sem, own_sem, send_sem, recv_sem, xres_sem,
           share_sem, every_sem, token):
    sizes, bands, width = plan.sizes, plan.bands, plan.width
    chunks, cut = plan.chunks, LANES
    tiles, row_tiles = width // LANES, bands // ROWS
    place = [lax.axis_index(axis) for axis in AXES]
    me_plane = place[0] * sizes[1] + place[1]
    me = me_plane * sizes[2] + place[2]

    def beside(d, step):
        return {AXES[d]: lax.rem(place[d] + step, sizes[d])}

    load = pltpu.make_async_copy(a_ref, own, own_sem)
    load.start()
    shifts = pltpu.make_async_copy(shift_hbm, shift_ref, shift_sem)
    shifts.start()

    barrier = pltpu.get_barrier_semaphore()
    for d in (2, 0, 1):
        source = beside(d, sizes[d] - plan.toward[d])
        pl.semaphore_signal(barrier, inc=1, device_id=source, device_id_type=MESH)
    pl.semaphore_wait(barrier, 3)

    def copy_of(d, c):
        return pltpu.make_async_remote_copy(
            src_ref=a_ref.at[:, pl.ds(pl.multiple_of(c * cut, cut), cut), :],
            dst_ref=partner.at[d, c],
            send_sem=send_sem.at[d],
            recv_sem=recv_sem.at[d, c],
            device_id=beside(d, plan.toward[d]),
            device_id_type=MESH,
        )

    last, parts = chunks - 1, plan.parts

    def tail_copy(part):
        low, span = parts[part]
        return pltpu.make_async_remote_copy(
            src_ref=a_ref.at[:, pl.ds(last * cut + low, span), :],
            dst_ref=partner.at[2, last, :, pl.ds(low, span), :],
            send_sem=send_sem.at[2],
            recv_sem=recv_sem.at[2, last + part],
            device_id=beside(2, plan.toward[2]),
            device_id_type=MESH,
        )

    def bulk(ref, semaphore):
        return pltpu.make_async_copy(ref, ref, semaphore)

    if plan.paired:
        computes = lax.rem(place[0] + place[1], 2) == 0
        yields = jnp.logical_not(computes)
    else:
        computes = yields = None

    def when(condition, act):
        if condition is None:
            act()
        else:
            pl.when(condition)(act)

    for c in range(last):
        copy_of(2, c).start()
    tail_copy(0).start()
    for c in range(chunks):
        when(yields, lambda: copy_of(0, c).start())
        copy_of(1, c).start()

    total[...] = jnp.zeros_like(total)
    diag_re[...] = jnp.zeros_like(diag_re)
    diag_im[...] = jnp.zeros_like(diag_im)
    rows[...] = jnp.zeros_like(rows)
    shifts.wait()
    load.wait()
    for d in range(3):
        if d == 0 and plan.paired:
            shift = jnp.where(place[d] == 0, tiles - shift_ref[d], shift_ref[d])
        elif d == 2:
            shift = jnp.where(place[d] == 0, tiles - shift_ref[d], 0)
        else:
            shift = jnp.where(place[d] == sizes[d] - 1, shift_ref[d], 0)
        moves = [(LANES << bit, (shift >> bit) & 1 == 1) for bit in range((tiles - 1).bit_length())]

        def turn(block, carry, d=d, moves=moves):
            strip = pl.ds(pl.multiple_of(block * STRIP, STRIP), STRIP)
            for part in range(2):
                value = own[part, strip, :]
                for amount, taken in moves:
                    moved = jnp.concatenate([value[:, width - amount:], value[:, :width - amount]], axis=1)
                    value = jnp.where(taken, moved, value)
                rolled[d, part, strip, :] = value
            return carry

        lax.fori_loop(0, bands // STRIP, turn, 0)

    for d in (1, 0, 2):
        for turn_no in range(sizes[d] - 1):
            pl.semaphore_signal(
                token.at[d], inc=1, device_id=beside(d, plan.toward[d]), device_id_type=MESH
            )
            pl.semaphore_wait(token.at[d], 1)

    row = lax.broadcasted_iota(jnp.int32, (ROWS, cut), 0)
    column = lax.broadcasted_iota(jnp.int32, (ROWS, cut), 1)

    def measure(slot, left_ref, d, c, start, count, lanes=(0, LANES)):
        low, span = lanes
        first = start if isinstance(start, int) else pl.multiple_of(start, count)
        left = left_ref[:, pl.ds(first, count), :].reshape(2 * count, width)
        right = partner[d, c, :, low:low + span].reshape(2 * span, width)
        product = lax.dot_general(left, right, (((1,), (1,)), ((), ())), preferred_element_type=jnp.float32)
        re = product[:count, :span] + product[count:, span:]
        im = product[:count, span:] - product[count:, :span]
        squares = re * re + im * im
        total[slot, :, :span] += jnp.sum(squares.reshape(count // 8, 8, span), axis=0)
        same = row[:count, :span] + start == column[:count, :span] + (c * cut + low)
        diag_re[slot, pl.ds(c, 1), low:low + span] += jnp.sum(jnp.where(same, re, 0.0), axis=0, keepdims=True)
        diag_im[slot, pl.ds(c, 1), low:low + span] += jnp.sum(jnp.where(same, im, 0.0), axis=0, keepdims=True)

    def whole(slot, left_ref, d, c, lanes=(0, LANES)):
        def one(r, carry):
            measure(slot, left_ref, d, c, r * ROWS, ROWS, lanes)
            return carry
        lax.fori_loop(0, row_tiles, one, 0)

    y_slot, z_slot = plan.slots - 2, plan.slots - 1

    def chunk(c, carry):
        copy_of(1, c).wait_recv()
        whole(y_slot, rolled.at[1], 1, c)

        def along_x():
            copy_of(0, c).wait_recv()
            if plan.paired:
                whole(0, own, 0, c)
                whole(1, rolled.at[0], 0, c)
            else:
                whole(0, rolled.at[0], 0, c)

        when(computes, along_x)
        return carry

    lax.fori_loop(0, chunks, chunk, 0)

    def phases(slot, sign=None):
        im = diag_im[slot] if sign is None else sign * diag_im[slot]
        return jnp.arctan2(im, diag_re[slot])

    xres_copy = pltpu.make_async_remote_copy(
        src_ref=xout, dst_ref=xres, send_sem=xres_sem.at[0], recv_sem=xres_sem.at[1],
        device_id=beside(0, sizes[0] - 1), device_id_type=MESH,
    )
    if plan.paired:
        def share_x():
            first = place[0] == 0
            sign = jnp.where(first, 1.0, -1.0)
            low, high = phases(0, sign), phases(1, -sign)
            xres[:chunks] = jnp.where(first, low, high)
            xres[chunks:] = jnp.where(first, total[0], total[1])
            xout[:chunks] = jnp.where(first, high, low)
            xout[chunks:] = jnp.where(first, total[1], total[0])
            xres_copy.start()

        pl.when(computes)(share_x)
    else:
        xres[:chunks] = phases(0)
        xres[chunks:] = total[0]

    def along_z(c, carry):
        copy_of(2, c).wait_recv()
        whole(z_slot, rolled.at[2], 2, c)
        return carry

    lax.fori_loop(0, last, along_z, 0)

    if plan.paired:
        pl.when(yields)(lambda: xres_copy.wait_recv())
    found = [xres[:chunks], phases(y_slot), phases(z_slot, -1.0)]
    for d in range(3):
        for c in range(chunks):
            if d * chunks + c < plan.rows - 1:
                rows[d * chunks + c] = found[d][c:c + 1]

    share, workers, plane = plan.share, plan.workers, plan.plane
    mine = pl.ds(me_plane * share, share)
    works, idles = me_plane < workers, me_plane >= workers

    def spot(p):
        return {"kx": p // sizes[1], "ky": p % sizes[1]}

    def pool_copy(source, worker):
        return pltpu.make_async_remote_copy(
            src_ref=rows.at[pl.ds(worker * share, share)], dst_ref=pooled.at[source],
            send_sem=share_sem.at[0], recv_sem=share_sem.at[1],
            device_id=spot(worker), device_id_type=MESH,
        )

    for worker in range(workers):
        pl.when(me_plane != worker)(lambda worker=worker: pool_copy(me_plane, worker).start())

    def level_copy(step):
        return pltpu.make_async_remote_copy(
            src_ref=levels.at[0], dst_ref=levels.at[step],
            send_sem=share_sem.at[2], recv_sem=share_sem.at[3],
            device_id=beside(2, step), device_id_type=MESH,
        )

    def final_copy(worker, p):
        return pltpu.make_async_remote_copy(
            src_ref=final.at[pl.ds(worker * share, share)], dst_ref=final.at[pl.ds(worker * share, share)],
            send_sem=share_sem.at[4], recv_sem=share_sem.at[5],
            device_id=spot(p), device_id_type=MESH,
        )

    def pool():
        pooled[me_plane] = rows[mine]
        bulk(pooled.at[pl.ds(0, plane - 1)], share_sem.at[1]).wait()
        mean = added([pooled[p] for p in range(plane)]) / plane
        square = added([(pooled[p] - mean) * (pooled[p] - mean) for p in range(plane)])
        levels[0, 0] = mean
        levels[0, 1] = square
        for step in range(1, sizes[2]):
            level_copy(step).start()

    def merge():
        bulk(levels.at[pl.ds(0, sizes[2] - 1)], share_sem.at[3]).wait()
        heard = []
        for z in range(sizes[2]):
            at = lax.rem(place[2] - z + sizes[2], sizes[2])
            heard.append((levels[at, 0], levels[at, 1]))
        mean = added([part[0] for part in heard]) / sizes[2]
        square = added([part[1] for part in heard])
        apart = added([(part[0] - mean) * (part[0] - mean) for part in heard])
        square = square + plane * apart
        for w in range(share):
            final[me_plane * share + w, 0] = mean[w]
            final[me_plane * share + w, 1] = square[w]
        for p in range(plane):
            pl.when(me_plane != p)(lambda p=p: final_copy(me_plane, p).start())

    pl.when(works)(pool)
    for part in range(1, len(parts)):
        tail_copy(part).start()
    pl.when(works)(merge)
    pl.when(works)(lambda: bulk(final.at[pl.ds(0, (workers - 1) * share)], share_sem.at[5]).wait())
    pl.when(idles)(lambda: bulk(final.at[pl.ds(0, workers * share)], share_sem.at[5]).wait())

    for r in range(plan.rows - 1):
        sums_ref[r:r + 1, :] = final[r, 0]
        sums_ref[plan.rows + r:plan.rows + r + 1, :] = final[r, 1]
    pl.when(works)(lambda: bulk(rows.at[pl.ds(0, (workers - 1) * share)], share_sem.at[0]).wait())
    pl.when(idles)(lambda: bulk(rows.at[pl.ds(0, workers * share)], share_sem.at[0]).wait())

    def settle():
        bulk(levels.at[pl.ds(0, sizes[2] - 1)], share_sem.at[2]).wait()
        bulk(final.at[pl.ds(0, (plane - 1) * share)], share_sem.at[4]).wait()

    pl.when(works)(settle)
    if plan.paired:
        pl.when(computes)(lambda: xres_copy.wait_send())
    when(yields, lambda: bulk(own, send_sem.at[0]).wait())
    bulk(own, send_sem.at[1]).wait()
    for part in range(len(parts) - 1):
        tail_copy(part).wait_recv()
        whole(z_slot, rolled.at[2], 2, last, parts[part])

    lanes = parts[-1]
    edge = bands - lanes[1]
    tail_copy(len(parts) - 1).wait_recv()
    measure(z_slot, rolled.at[2], 2, last, edge, lanes[1], lanes)
    every[me] = jnp.arctan2(-diag_im[z_slot, last:last + 1], diag_re[z_slot, last:last + 1])

    def place_of(k):
        return (k // sizes[1]) % sizes[0], k % sizes[1], k // plane

    def slot_of(k):
        x, y, z = place_of(k)
        return (x * sizes[1] + y) * sizes[2] + z

    def every_copy(k):
        x, y, z = place_of(k)
        return pltpu.make_async_remote_copy(
            src_ref=every.at[me], dst_ref=every.at[me],
            send_sem=every_sem.at[0], recv_sem=every_sem.at[1],
            device_id={"kx": x, "ky": y, "kz": z}, device_id_type=MESH,
        )

    few = plan.devices <= 64

    def each(act):
        def one(k, carry=0):
            pl.when(me != slot_of(k))(lambda: act(k))
            return carry
        if few:
            for k in range(plan.devices):
                one(k)
        else:
            lax.fori_loop(0, plan.devices, one, 0)

    each(lambda k: every_copy(k).start())
    for start in range(0, edge, ROWS):
        measure(z_slot, rolled.at[2], 2, last, start, min(ROWS, edge - start), lanes)
    ztotal_copy = pltpu.make_async_remote_copy(
        src_ref=total.at[z_slot], dst_ref=ztotal, send_sem=xres_sem.at[2], recv_sem=xres_sem.at[3],
        device_id=beside(2, sizes[2] - plan.toward[2]), device_id_type=MESH,
    )
    ztotal_copy.start()
    at = 2 * plan.rows
    sums_ref[at:at + 8, :] = xres[chunks:]
    sums_ref[at + 8:at + 16, :] = total[y_slot]
    bulk(own, send_sem.at[2]).wait()
    others = every.at[pl.ds(0, plan.devices - 1)]
    bulk(others, every_sem.at[0]).wait()
    ztotal_copy.wait_send()
    ztotal_copy.wait_recv()
    sums_ref[at + 16:at + 24, :] = ztotal[...]

    bulk(others, every_sem.at[1]).wait()
    if few:
        heard = [every[k] for k in range(plan.devices)]
        mean = added(heard) / plan.devices
        square = added([(phase - mean) * (phase - mean) for phase in heard])
    else:
        zero = jnp.zeros((1, cut), jnp.float32)
        mean = lax.fori_loop(0, plan.devices, lambda k, sofar: sofar + every[k], zero) / plan.devices
        square = lax.fori_loop(
            0, plan.devices, lambda k, sofar: sofar + (every[k] - mean) * (every[k] - mean), zero
        )
    sums_ref[plan.rows - 1:plan.rows, :] = mean
    sums_ref[2 * plan.rows - 1:2 * plan.rows, :] = square


def results(plan, sums_ref, centre_ref, spread_ref, coherence_ref):
    chunks, count = plan.chunks, plan.devices
    for d in range(3):
        scale = plan.sizes[d] / (2.0 * jnp.pi)
        for c in range(chunks):
            lanes = slice(c * LANES, (c + 1) * LANES)
            at = d * chunks + c
            centre_ref[d:d + 1, lanes] = -scale * sums_ref[at:at + 1, :]
            at += plan.rows
            spread_ref[d:d + 1, lanes] = scale * scale * (sums_ref[at:at + 1, :] / count)
    for d in range(3):
        at = 2 * plan.rows + 8 * d
        coherence_ref[d] = jnp.sum(sums_ref[at:at + 8, :]) / plan.bands


def solution(mesh):
    sizes = tuple(mesh.shape[axis] for axis in AXES)

    def shards(coefficients, shift_blocks):
        bands, width = coefficients.shape[4], coefficients.shape[5]
        plan = Plan(sizes, bands, width)
        chunks = plan.chunks
        vmem = pl.BlockSpec(memory_space=pltpu.VMEM)
        hbm = pl.BlockSpec(memory_space=pl.ANY)
        dma = pltpu.SemaphoreType.DMA
        padded = plan.plane * plan.share
        sums = pl.pallas_call(
            functools.partial(kernel, plan),
            out_shape=pltpu.VMEM((2 * plan.rows + 24, LANES), jnp.float32),
            in_specs=[hbm, hbm],
            out_specs=vmem,
            scratch_shapes=[
                pltpu.SMEM((3,), jnp.int32),
                pltpu.VMEM((2, bands, width), jnp.bfloat16),
                pltpu.VMEM((3, chunks, 2, LANES, width), jnp.bfloat16),
                pltpu.VMEM((3, 2, bands, width), jnp.bfloat16),
                pltpu.VMEM((plan.slots, chunks, LANES), jnp.float32),
                pltpu.VMEM((plan.slots, chunks, LANES), jnp.float32),
                pltpu.VMEM((plan.slots, 8, LANES), jnp.float32),
                pltpu.VMEM((chunks + 8, LANES), jnp.float32),
                pltpu.VMEM((chunks + 8, LANES), jnp.float32),
                pltpu.VMEM((8, LANES), jnp.float32),
                pltpu.VMEM((padded, 1, LANES), jnp.float32),
                pltpu.VMEM((plan.plane, plan.share, 1, LANES), jnp.float32),
                pltpu.VMEM((sizes[2], 2, plan.share, 1, LANES), jnp.float32),
                pltpu.VMEM((padded, 2, 1, LANES), jnp.float32),
                pltpu.VMEM((plan.devices, 1, LANES), jnp.float32),
                dma,
                dma,
                dma((3,)),
                dma((3, chunks + len(plan.parts) - 1)),
                dma((4,)),
                dma((6,)),
                dma((2,)),
                pltpu.SemaphoreType.REGULAR((3,)),
            ],
            compiler_params=pltpu.CompilerParams(
                collective_id=0, has_side_effects=True, vmem_limit_bytes=60 * 1024 * 1024
            ),
        )(shift_blocks, coefficients.reshape(2, bands, width))
        sums = pltpu.with_memory_space_constraint(sums, pltpu.VMEM)
        centre, spread, coherence = pl.pallas_call(
            functools.partial(results, plan),
            out_shape=(
                jax.ShapeDtypeStruct((3, bands), jnp.float32),
                jax.ShapeDtypeStruct((3, bands), jnp.float32),
                jax.ShapeDtypeStruct((3,), jnp.float32),
            ),
            in_specs=[vmem],
            out_specs=(vmem, vmem, pl.BlockSpec(memory_space=pltpu.SMEM)),
        )(sums)
        return centre, spread, coherence.reshape(3, 1, 1, 1)

    in_specs = (P(None, "kx", "ky", "kz", None, None), P())
    out_specs = (P(), P(), P(None, "kx", "ky", "kz"))
    return jax.shard_map(shards, mesh=mesh, in_specs=in_specs, out_specs=out_specs, check_vma=False)
```

```python
import functools

import jax
import jax.numpy as jnp
from jax import lax
from jax.experimental import pallas as pl
from jax.experimental.pallas import tpu as pltpu
from jax.sharding import PartitionSpec as P

MESH = pl.DeviceIdType.MESH
AXES = ("kx", "ky", "kz")
LANES = 128
ROWS = 256
STRIP = 32


def added(parts):
    while len(parts) > 1:
        parts = [a + b for a, b in zip(parts[::2], parts[1::2])] + parts[len(parts) // 2 * 2:]
    return parts[0]


class Plan:
    def __init__(self, sizes, bands, width):
        self.sizes = sizes
        self.bands, self.width = bands, width
        self.paired = sizes[0] == 2
        self.chunks = bands // LANES
        self.rows = 3 * self.chunks
        self.plane = sizes[0] * sizes[1]
        self.share = -(-self.rows // self.plane)
        self.workers = -(-(self.rows - 1) // self.share)
        self.devices = self.plane * sizes[2]
        self.slots = 4 if self.paired else 3
        self.toward = [sizes[0] - 1, sizes[1] - 1, 1]
        self.parts = ((0, 64), (64, 32), (96, 32))


def kernel(plan, shift_hbm, a_ref, centre_ref, spread_ref, coherence_ref,
           shift_ref, own, partner, rolled, diag_re, diag_im, total,
           xres, xout, ztotal, rows, pooled, levels, final, every,
           shift_sem, own_sem, send_sem, recv_sem, xres_sem,
           share_sem, every_sem, token):
    sizes, bands, width = plan.sizes, plan.bands, plan.width
    chunks, cut = plan.chunks, LANES
    tiles, row_tiles = width // LANES, bands // ROWS
    place = [lax.axis_index(axis) for axis in AXES]
    me_plane = place[0] * sizes[1] + place[1]
    me = me_plane * sizes[2] + place[2]

    def beside(d, step):
        return {AXES[d]: lax.rem(place[d] + step, sizes[d])}

    def load(k):
        low, span = ((0, cut), (cut, bands - cut))[k]
        piece = pl.ds(low, span)
        return pltpu.make_async_copy(a_ref.at[:, piece, :], own.at[:, piece, :], own_sem.at[k])

    barrier = pltpu.get_barrier_semaphore()
    for d in (2, 0, 1):
        source = beside(d, sizes[d] - plan.toward[d])
        pl.semaphore_signal(barrier, inc=1, device_id=source, device_id_type=MESH)
    for k in range(2):
        load(k).start()
    shifts = pltpu.make_async_copy(shift_hbm, shift_ref, shift_sem)
    shifts.start()
    pl.semaphore_wait(barrier, 3)

    def rows_of(c):
        return pl.ds(pl.multiple_of(c * cut, cut), cut)

    def copy_of(d, c):
        return pltpu.make_async_remote_copy(
            src_ref=(own if d == 2 and isinstance(c, int) and c == 0 else a_ref).at[:, rows_of(c), :],
            dst_ref=partner.at[d, c],
            send_sem=send_sem.at[d],
            recv_sem=recv_sem.at[d, c],
            device_id=beside(d, plan.toward[d]),
            device_id_type=MESH,
        )

    last, parts = chunks - 1, plan.parts

    def tail_copy(part):
        low, span = parts[part]
        return pltpu.make_async_remote_copy(
            src_ref=a_ref.at[:, pl.ds(last * cut + low, span), :],
            dst_ref=partner.at[2, last, :, pl.ds(low, span), :],
            send_sem=send_sem.at[2],
            recv_sem=recv_sem.at[2, last + part],
            device_id=beside(2, plan.toward[2]),
            device_id_type=MESH,
        )

    def bulk(ref, semaphore):
        return pltpu.make_async_copy(ref, ref, semaphore)

    if plan.paired:
        computes = lax.rem(place[0] + place[1], 2) == 0
        yields = jnp.logical_not(computes)
    else:
        computes = yields = None

    def when(condition, act):
        if condition is None:
            act()
        else:
            pl.when(condition)(act)

    load(0).wait()
    for c in range(last):
        copy_of(2, c).start()
    tail_copy(0).start()
    for c in range(chunks):
        when(yields, lambda: copy_of(0, c).start())
        copy_of(1, c).start()

    total[...] = jnp.zeros_like(total)
    diag_re[...] = jnp.zeros_like(diag_re)
    diag_im[...] = jnp.zeros_like(diag_im)
    rows[...] = jnp.zeros_like(rows)
    shifts.wait()
    load(1).wait()
    for d in range(3):
        if d == 0 and plan.paired:
            shift = jnp.where(place[d] == 0, tiles - shift_ref[d], shift_ref[d])
        elif d == 2:
            shift = jnp.where(place[d] == 0, tiles - shift_ref[d], 0)
        else:
            shift = jnp.where(place[d] == sizes[d] - 1, shift_ref[d], 0)
        moves = [(LANES << bit, (shift >> bit) & 1 == 1) for bit in range((tiles - 1).bit_length())]

        def turn(block, carry, d=d, moves=moves):
            strip = pl.ds(pl.multiple_of(block * STRIP, STRIP), STRIP)
            for part in range(2):
                value = own[part, strip, :]
                for amount, taken in moves:
                    moved = jnp.concatenate([value[:, width - amount:], value[:, :width - amount]], axis=1)
                    value = jnp.where(taken, moved, value)
                rolled[d, part, strip, :] = value
            return carry

        lax.fori_loop(0, bands // STRIP, turn, 0)

    for d in (1, 0, 2):
        for turn_no in range(sizes[d] - 1):
            pl.semaphore_signal(
                token.at[d], inc=1, device_id=beside(d, plan.toward[d]), device_id_type=MESH
            )
            pl.semaphore_wait(token.at[d], 1)

    row = lax.broadcasted_iota(jnp.int32, (ROWS, cut), 0)
    column = lax.broadcasted_iota(jnp.int32, (ROWS, cut), 1)

    def measure(slot, left_ref, d, c, start, count, lanes=(0, LANES)):
        low, span = lanes
        first = start if isinstance(start, int) else pl.multiple_of(start, count)
        left = left_ref[:, pl.ds(first, count), :].reshape(2 * count, width)
        right = partner[d, c, :, low:low + span].reshape(2 * span, width)
        product = lax.dot_general(left, right, (((1,), (1,)), ((), ())), preferred_element_type=jnp.float32)
        re = product[:count, :span] + product[count:, span:]
        im = product[:count, span:] - product[count:, :span]
        squares = re * re + im * im
        total[slot, :, :span] += jnp.sum(squares.reshape(count // 8, 8, span), axis=0)
        same = row[:count, :span] + start == column[:count, :span] + (c * cut + low)
        diag_re[slot, pl.ds(c, 1), low:low + span] += jnp.sum(jnp.where(same, re, 0.0), axis=0, keepdims=True)
        diag_im[slot, pl.ds(c, 1), low:low + span] += jnp.sum(jnp.where(same, im, 0.0), axis=0, keepdims=True)

    def whole(slot, left_ref, d, c, lanes=(0, LANES)):
        def one(r, carry):
            measure(slot, left_ref, d, c, r * ROWS, ROWS, lanes)
            return carry
        lax.fori_loop(0, row_tiles, one, 0)

    y_slot, z_slot = plan.slots - 2, plan.slots - 1

    def chunk(c, carry):
        copy_of(1, c).wait_recv()
        whole(y_slot, rolled.at[1], 1, c)

        def along_x():
            copy_of(0, c).wait_recv()
            if plan.paired:
                whole(0, own, 0, c)
                whole(1, rolled.at[0], 0, c)
            else:
                whole(0, rolled.at[0], 0, c)

        when(computes, along_x)
        return carry

    lax.fori_loop(0, chunks, chunk, 0)

    def phases(slot, sign=None):
        im = diag_im[slot] if sign is None else sign * diag_im[slot]
        return jnp.arctan2(im, diag_re[slot])

    xres_copy = pltpu.make_async_remote_copy(
        src_ref=xout, dst_ref=xres, send_sem=xres_sem.at[0], recv_sem=xres_sem.at[1],
        device_id=beside(0, sizes[0] - 1), device_id_type=MESH,
    )
    if plan.paired:
        def share_x():
            first = place[0] == 0
            sign = jnp.where(first, 1.0, -1.0)
            low, high = phases(0, sign), phases(1, -sign)
            xres[:chunks] = jnp.where(first, low, high)
            xres[chunks:] = jnp.where(first, total[0], total[1])
            xout[:chunks] = jnp.where(first, high, low)
            xout[chunks:] = jnp.where(first, total[1], total[0])
            xres_copy.start()

        pl.when(computes)(share_x)
    else:
        xres[:chunks] = phases(0)
        xres[chunks:] = total[0]

    def along_z(c, carry):
        copy_of(2, c).wait_recv()
        whole(z_slot, rolled.at[2], 2, c)
        return carry

    lax.fori_loop(0, last, along_z, 0)

    if plan.paired:
        pl.when(yields)(lambda: xres_copy.wait_recv())
    found = [xres[:chunks], phases(y_slot), phases(z_slot, -1.0)]
    for d in range(3):
        for c in range(chunks):
            if d * chunks + c < plan.rows - 1:
                rows[d * chunks + c] = found[d][c:c + 1]

    share, workers, plane = plan.share, plan.workers, plan.plane
    mine = pl.ds(me_plane * share, share)
    works, idles = me_plane < workers, me_plane >= workers

    def spot(p):
        return {"kx": p // sizes[1], "ky": p % sizes[1]}

    def pool_copy(source, worker):
        return pltpu.make_async_remote_copy(
            src_ref=rows.at[pl.ds(worker * share, share)], dst_ref=pooled.at[source],
            send_sem=share_sem.at[0], recv_sem=share_sem.at[1],
            device_id=spot(worker), device_id_type=MESH,
        )

    for worker in range(workers):
        pl.when(me_plane != worker)(lambda worker=worker: pool_copy(me_plane, worker).start())

    def level_copy(step):
        return pltpu.make_async_remote_copy(
            src_ref=levels.at[0], dst_ref=levels.at[step],
            send_sem=share_sem.at[2], recv_sem=share_sem.at[3],
            device_id=beside(2, step), device_id_type=MESH,
        )

    def final_copy(worker, p):
        return pltpu.make_async_remote_copy(
            src_ref=final.at[pl.ds(worker * share, share)], dst_ref=final.at[pl.ds(worker * share, share)],
            send_sem=share_sem.at[4], recv_sem=share_sem.at[5],
            device_id=spot(p), device_id_type=MESH,
        )

    def pool():
        pooled[me_plane] = rows[mine]
        bulk(pooled.at[pl.ds(0, plane - 1)], share_sem.at[1]).wait()
        mean = added([pooled[p] for p in range(plane)]) / plane
        square = added([(pooled[p] - mean) * (pooled[p] - mean) for p in range(plane)])
        levels[0, 0] = mean
        levels[0, 1] = square
        for step in range(1, sizes[2]):
            level_copy(step).start()

    def merge():
        bulk(levels.at[pl.ds(0, sizes[2] - 1)], share_sem.at[3]).wait()
        heard = []
        for z in range(sizes[2]):
            at = lax.rem(place[2] - z + sizes[2], sizes[2])
            heard.append((levels[at, 0], levels[at, 1]))
        mean = added([part[0] for part in heard]) / sizes[2]
        square = added([part[1] for part in heard])
        apart = added([(part[0] - mean) * (part[0] - mean) for part in heard])
        square = square + plane * apart
        for w in range(share):
            final[me_plane * share + w, 0] = mean[w]
            final[me_plane * share + w, 1] = square[w]
        for p in range(plane):
            pl.when(me_plane != p)(lambda p=p: final_copy(me_plane, p).start())

    pl.when(works)(pool)
    for part in range(1, len(parts)):
        tail_copy(part).start()
    pl.when(works)(merge)
    pl.when(works)(lambda: bulk(final.at[pl.ds(0, (workers - 1) * share)], share_sem.at[5]).wait())
    pl.when(idles)(lambda: bulk(final.at[pl.ds(0, workers * share)], share_sem.at[5]).wait())

    def settled(r, mean, square):
        d, lanes = r // chunks, slice(r % chunks * cut, (r % chunks + 1) * cut)
        scale = sizes[d] / (2.0 * jnp.pi)
        centre_ref[d:d + 1, lanes] = -scale * mean
        spread_ref[d:d + 1, lanes] = scale * scale * (square / plan.devices)

    def norm(squares):
        return jnp.sum(jnp.sum(squares, axis=0, keepdims=True), axis=1, keepdims=True) / bands

    for r in range(plan.rows - 1):
        settled(r, final[r, 0], final[r, 1])
    coherence_ref[:, 0:1] = norm(xres[chunks:])
    coherence_ref[:, 1:2] = norm(total[y_slot])
    pl.when(works)(lambda: bulk(rows.at[pl.ds(0, (workers - 1) * share)], share_sem.at[0]).wait())
    pl.when(idles)(lambda: bulk(rows.at[pl.ds(0, workers * share)], share_sem.at[0]).wait())

    def settle():
        bulk(levels.at[pl.ds(0, sizes[2] - 1)], share_sem.at[2]).wait()
        bulk(final.at[pl.ds(0, (plane - 1) * share)], share_sem.at[4]).wait()

    pl.when(works)(settle)
    if plan.paired:
        pl.when(computes)(lambda: xres_copy.wait_send())
    when(yields, lambda: bulk(own, send_sem.at[0]).wait())
    bulk(own, send_sem.at[1]).wait()
    for part in range(len(parts) - 1):
        tail_copy(part).wait_recv()
        whole(z_slot, rolled.at[2], 2, last, parts[part])

    lanes = parts[-1]
    edge = bands - lanes[1]
    tail_copy(len(parts) - 1).wait_recv()
    measure(z_slot, rolled.at[2], 2, last, edge, lanes[1], lanes)
    every[me] = jnp.arctan2(-diag_im[z_slot, last:last + 1], diag_re[z_slot, last:last + 1])

    def place_of(k):
        return (k // sizes[1]) % sizes[0], k % sizes[1], k // plane

    def slot_of(k):
        x, y, z = place_of(k)
        return (x * sizes[1] + y) * sizes[2] + z

    def every_copy(k):
        x, y, z = place_of(k)
        return pltpu.make_async_remote_copy(
            src_ref=every.at[me], dst_ref=every.at[me],
            send_sem=every_sem.at[0], recv_sem=every_sem.at[1],
            device_id={"kx": x, "ky": y, "kz": z}, device_id_type=MESH,
        )

    few = plan.devices <= 64

    def each(act):
        def one(k, carry=0):
            pl.when(me != slot_of(k))(lambda: act(k))
            return carry
        if few:
            for k in range(plan.devices):
                one(k)
        else:
            lax.fori_loop(0, plan.devices, one, 0)

    each(lambda k: every_copy(k).start())
    for start in range(0, edge, ROWS):
        measure(z_slot, rolled.at[2], 2, last, start, min(ROWS, edge - start), lanes)
    ztotal_copy = pltpu.make_async_remote_copy(
        src_ref=total.at[z_slot], dst_ref=ztotal, send_sem=xres_sem.at[2], recv_sem=xres_sem.at[3],
        device_id=beside(2, sizes[2] - plan.toward[2]), device_id_type=MESH,
    )
    ztotal_copy.start()
    bulk(own, send_sem.at[2]).wait()
    others = every.at[pl.ds(0, plan.devices - 1)]
    bulk(others, every_sem.at[0]).wait()
    ztotal_copy.wait_send()
    ztotal_copy.wait_recv()
    coherence_ref[:, 2:3] = norm(ztotal[...])

    bulk(others, every_sem.at[1]).wait()
    if few:
        heard = [every[k] for k in range(plan.devices)]
        mean = added(heard) / plan.devices
        square = added([(phase - mean) * (phase - mean) for phase in heard])
    else:
        zero = jnp.zeros((1, cut), jnp.float32)
        mean = lax.fori_loop(0, plan.devices, lambda k, sofar: sofar + every[k], zero) / plan.devices
        square = lax.fori_loop(
            0, plan.devices, lambda k, sofar: sofar + (every[k] - mean) * (every[k] - mean), zero
        )
    settled(plan.rows - 1, mean, square)


def results(held_centre, held_spread, held_coherence, centre_ref, spread_ref, coherence_ref, sems):
    pairs = ((held_centre, centre_ref), (held_spread, spread_ref), (held_coherence, coherence_ref))
    copies = [pltpu.make_async_copy(held, out, sems.at[k]) for k, (held, out) in enumerate(pairs)]
    for copy in copies:
        copy.start()
    for copy in copies:
        copy.wait()


def solution(mesh):
    sizes = tuple(mesh.shape[axis] for axis in AXES)

    def shards(coefficients, shift_blocks):
        bands, width = coefficients.shape[4], coefficients.shape[5]
        plan = Plan(sizes, bands, width)
        chunks = plan.chunks
        vmem = pl.BlockSpec(memory_space=pltpu.VMEM)
        hbm = pl.BlockSpec(memory_space=pl.ANY)
        dma = pltpu.SemaphoreType.DMA
        padded = plan.plane * plan.share
        shapes = ((3, bands), (3, bands), (1, 3))
        held = pl.pallas_call(
            functools.partial(kernel, plan),
            out_shape=tuple(pltpu.VMEM(shape, jnp.float32) for shape in shapes),
            in_specs=[hbm, hbm],
            out_specs=(vmem, vmem, vmem),
            scratch_shapes=[
                pltpu.SMEM((3,), jnp.int32),
                pltpu.VMEM((2, bands, width), jnp.bfloat16),
                pltpu.VMEM((3, chunks, 2, LANES, width), jnp.bfloat16),
                pltpu.VMEM((3, 2, bands, width), jnp.bfloat16),
                pltpu.VMEM((plan.slots, chunks, LANES), jnp.float32),
                pltpu.VMEM((plan.slots, chunks, LANES), jnp.float32),
                pltpu.VMEM((plan.slots, 8, LANES), jnp.float32),
                pltpu.VMEM((chunks + 8, LANES), jnp.float32),
                pltpu.VMEM((chunks + 8, LANES), jnp.float32),
                pltpu.VMEM((8, LANES), jnp.float32),
                pltpu.VMEM((padded, 1, LANES), jnp.float32),
                pltpu.VMEM((plan.plane, plan.share, 1, LANES), jnp.float32),
                pltpu.VMEM((sizes[2], 2, plan.share, 1, LANES), jnp.float32),
                pltpu.VMEM((padded, 2, 1, LANES), jnp.float32),
                pltpu.VMEM((plan.devices, 1, LANES), jnp.float32),
                dma,
                dma((2,)),
                dma((3,)),
                dma((3, chunks + len(plan.parts) - 1)),
                dma((4,)),
                dma((6,)),
                dma((2,)),
                pltpu.SemaphoreType.REGULAR((3,)),
            ],
            compiler_params=pltpu.CompilerParams(
                collective_id=0, has_side_effects=True, vmem_limit_bytes=60 * 1024 * 1024
            ),
        )(shift_blocks, coefficients.reshape(2, bands, width))
        held = [pltpu.with_memory_space_constraint(array, pltpu.VMEM) for array in held]
        centre, spread, coherence = pl.pallas_call(
            results,
            out_shape=tuple(jax.ShapeDtypeStruct(shape, jnp.float32) for shape in shapes),
            in_specs=[vmem, vmem, vmem],
            out_specs=(hbm, hbm, hbm),
            scratch_shapes=[dma((3,))],
        )(*held)
        return centre, spread, coherence.reshape(3, 1, 1, 1)

    in_specs = (P(None, "kx", "ky", "kz", None, None), P())
    out_specs = (P(), P(), P(None, "kx", "ky", "kz"))
    return jax.shard_map(shards, mesh=mesh, in_specs=in_specs, out_specs=out_specs, check_vma=False)
```

```python
import functools

import jax
import jax.numpy as jnp
from jax import lax
from jax.experimental import pallas as pl
from jax.experimental.pallas import tpu as pltpu
from jax.sharding import PartitionSpec as P

MESH = pl.DeviceIdType.MESH
AXES = ("kx", "ky", "kz")
LANES = 128
ROWS = 256
STRIP = 32


def added(parts):
    while len(parts) > 1:
        parts = [a + b for a, b in zip(parts[::2], parts[1::2])] + parts[len(parts) // 2 * 2:]
    return parts[0]


class Plan:
    def __init__(self, sizes, bands, width):
        self.sizes = sizes
        self.bands, self.width = bands, width
        self.paired = sizes[0] == 2
        self.chunks = bands // LANES
        self.rows = 3 * self.chunks
        self.plane = sizes[0] * sizes[1]
        self.share = -(-self.rows // self.plane)
        self.workers = -(-(self.rows - 1) // self.share)
        self.devices = self.plane * sizes[2]
        self.slots = 4 if self.paired else 3
        self.toward = [sizes[0] - 1, sizes[1] - 1, 1]
        self.parts = ((0, 64), (64, 32), (96, 32))


def kernel(plan, shift_hbm, a_ref, centre_ref, spread_ref, coherence_ref,
           shift_ref, own, partner, rolled, diag_re, diag_im, total,
           xres, xout, ztotal, rows, pooled, levels, final, every,
           shift_sem, own_sem, send_sem, recv_sem, xres_sem,
           share_sem, every_sem, token):
    sizes, bands, width = plan.sizes, plan.bands, plan.width
    chunks, cut = plan.chunks, LANES
    tiles, row_tiles = width // LANES, bands // ROWS
    place = [lax.axis_index(axis) for axis in AXES]
    me_plane = place[0] * sizes[1] + place[1]
    me = me_plane * sizes[2] + place[2]

    def beside(d, step):
        return {AXES[d]: lax.rem(place[d] + step, sizes[d])}

    def load(k):
        low, span = ((0, cut), (cut, bands - cut))[k]
        piece = pl.ds(low, span)
        return pltpu.make_async_copy(a_ref.at[:, piece, :], own.at[:, piece, :], own_sem.at[k])

    barrier = pltpu.get_barrier_semaphore()
    top = place[2] == sizes[2] - 1
    below = place[2] == sizes[2] - 2
    lower = place[2] < sizes[2] - 1

    def source(d):
        return beside(d, sizes[d] - plan.toward[d])

    pl.semaphore_signal(barrier, inc=1, device_id=source(2), device_id_type=MESH)

    def greet():
        for d in range(2):
            pl.semaphore_signal(barrier, inc=1, device_id=source(d), device_id_type=MESH)

    pl.when(lower)(greet)
    for k in range(2):
        load(k).start()
    shifts = pltpu.make_async_copy(shift_hbm, shift_ref, shift_sem)
    shifts.start()
    pl.when(lower)(lambda: pl.semaphore_wait(barrier, 3))
    pl.when(top)(lambda: pl.semaphore_wait(barrier, 1))

    def rows_of(c):
        return pl.ds(pl.multiple_of(c * cut, cut), cut)

    def copy_of(d, c, held=False):
        return pltpu.make_async_remote_copy(
            src_ref=(own if held else a_ref).at[:, rows_of(c), :],
            dst_ref=partner.at[d, c],
            send_sem=send_sem.at[d],
            recv_sem=recv_sem.at[d, c],
            device_id=beside(d, plan.toward[d]),
            device_id_type=MESH,
        )

    last, parts = chunks - 1, plan.parts

    def tail_copy(part):
        low, span = parts[part]
        return pltpu.make_async_remote_copy(
            src_ref=a_ref.at[:, pl.ds(last * cut + low, span), :],
            dst_ref=partner.at[2, last, :, pl.ds(low, span), :],
            send_sem=send_sem.at[2],
            recv_sem=recv_sem.at[2, last + part],
            device_id=beside(2, plan.toward[2]),
            device_id_type=MESH,
        )

    def bulk(ref, semaphore):
        return pltpu.make_async_copy(ref, ref, semaphore)

    if plan.paired:
        computes = lax.rem(place[0] + place[1], 2) == 0
        yields = jnp.logical_not(computes)
    else:
        computes = yields = None

    def when(condition, act):
        if condition is None:
            act()
        else:
            pl.when(condition)(act)

    def begin():
        load(0).wait()
        copy_of(2, 0, True).start()

    pl.when(lower)(begin)
    pl.when(top)(lambda: copy_of(2, 0).start())
    for c in range(1, last):
        copy_of(2, c).start()
    tail_copy(0).start()
    def across():
        for c in range(chunks):
            when(yields, lambda: copy_of(0, c).start())
            copy_of(1, c).start()

    def pass_on(d):
        for turn_no in range(sizes[d] - 1):
            pl.semaphore_signal(
                token.at[d], inc=1, device_id=beside(d, plan.toward[d]), device_id_type=MESH
            )
            pl.semaphore_wait(token.at[d], 1)

    def spread():
        across()
        pass_on(1)
        pass_on(0)

    def relay():
        pl.semaphore_signal(token.at[3], inc=1, device_id=beside(2, 1), device_id_type=MESH)

    pl.when(lower)(spread)
    pl.when(below)(relay)

    def follow():
        pl.semaphore_wait(token.at[3], 1)
        across()

    pl.when(top)(follow)

    total[...] = jnp.zeros_like(total)
    diag_re[...] = jnp.zeros_like(diag_re)
    diag_im[...] = jnp.zeros_like(diag_im)
    rows[...] = jnp.zeros_like(rows)
    shifts.wait()
    pl.when(top)(lambda: load(0).wait())
    load(1).wait()
    for d in range(3):
        if d == 0 and plan.paired:
            shift = jnp.where(place[d] == 0, tiles - shift_ref[d], shift_ref[d])
        elif d == 2:
            shift = jnp.where(place[d] == 0, tiles - shift_ref[d], 0)
        else:
            shift = jnp.where(place[d] == sizes[d] - 1, shift_ref[d], 0)
        moves = [(LANES << bit, (shift >> bit) & 1 == 1) for bit in range((tiles - 1).bit_length())]

        def turn(block, carry, d=d, moves=moves):
            strip = pl.ds(pl.multiple_of(block * STRIP, STRIP), STRIP)
            for part in range(2):
                value = own[part, strip, :]
                for amount, taken in moves:
                    moved = jnp.concatenate([value[:, width - amount:], value[:, :width - amount]], axis=1)
                    value = jnp.where(taken, moved, value)
                rolled[d, part, strip, :] = value
            return carry

        lax.fori_loop(0, bands // STRIP, turn, 0)

    pass_on(2)

    row = lax.broadcasted_iota(jnp.int32, (ROWS, cut), 0)
    column = lax.broadcasted_iota(jnp.int32, (ROWS, cut), 1)

    def measure(slot, left_ref, d, c, start, count, lanes=(0, LANES)):
        low, span = lanes
        first = start if isinstance(start, int) else pl.multiple_of(start, count)
        left = left_ref[:, pl.ds(first, count), :].reshape(2 * count, width)
        right = partner[d, c, :, low:low + span].reshape(2 * span, width)
        product = lax.dot_general(left, right, (((1,), (1,)), ((), ())), preferred_element_type=jnp.float32)
        re = product[:count, :span] + product[count:, span:]
        im = product[:count, span:] - product[count:, :span]
        squares = re * re + im * im
        total[slot, :, :span] += jnp.sum(squares.reshape(count // 8, 8, span), axis=0)
        same = row[:count, :span] + start == column[:count, :span] + (c * cut + low)
        diag_re[slot, pl.ds(c, 1), low:low + span] += jnp.sum(jnp.where(same, re, 0.0), axis=0, keepdims=True)
        diag_im[slot, pl.ds(c, 1), low:low + span] += jnp.sum(jnp.where(same, im, 0.0), axis=0, keepdims=True)

    def whole(slot, left_ref, d, c, lanes=(0, LANES)):
        def one(r, carry):
            measure(slot, left_ref, d, c, r * ROWS, ROWS, lanes)
            return carry
        lax.fori_loop(0, row_tiles, one, 0)

    y_slot, z_slot = plan.slots - 2, plan.slots - 1

    def chunk(c, carry):
        copy_of(1, c).wait_recv()
        whole(y_slot, rolled.at[1], 1, c)

        def along_x():
            copy_of(0, c).wait_recv()
            if plan.paired:
                whole(0, own, 0, c)
                whole(1, rolled.at[0], 0, c)
            else:
                whole(0, rolled.at[0], 0, c)

        when(computes, along_x)
        return carry

    lax.fori_loop(0, chunks, chunk, 0)

    def phases(slot, sign=None):
        im = diag_im[slot] if sign is None else sign * diag_im[slot]
        return jnp.arctan2(im, diag_re[slot])

    xres_copy = pltpu.make_async_remote_copy(
        src_ref=xout, dst_ref=xres, send_sem=xres_sem.at[0], recv_sem=xres_sem.at[1],
        device_id=beside(0, sizes[0] - 1), device_id_type=MESH,
    )
    if plan.paired:
        def share_x():
            first = place[0] == 0
            sign = jnp.where(first, 1.0, -1.0)
            low, high = phases(0, sign), phases(1, -sign)
            xres[:chunks] = jnp.where(first, low, high)
            xres[chunks:] = jnp.where(first, total[0], total[1])
            xout[:chunks] = jnp.where(first, high, low)
            xout[chunks:] = jnp.where(first, total[1], total[0])
            xres_copy.start()

        pl.when(computes)(share_x)
    else:
        xres[:chunks] = phases(0)
        xres[chunks:] = total[0]

    def along_z(c, carry):
        copy_of(2, c).wait_recv()
        whole(z_slot, rolled.at[2], 2, c)
        return carry

    lax.fori_loop(0, last, along_z, 0)

    if plan.paired:
        pl.when(yields)(lambda: xres_copy.wait_recv())
    found = [xres[:chunks], phases(y_slot), phases(z_slot, -1.0)]
    for d in range(3):
        for c in range(chunks):
            if d * chunks + c < plan.rows - 1:
                rows[d * chunks + c] = found[d][c:c + 1]

    share, workers, plane = plan.share, plan.workers, plan.plane
    mine = pl.ds(me_plane * share, share)
    works, idles = me_plane < workers, me_plane >= workers

    def spot(p):
        return {"kx": p // sizes[1], "ky": p % sizes[1]}

    def pool_copy(source, worker):
        return pltpu.make_async_remote_copy(
            src_ref=rows.at[pl.ds(worker * share, share)], dst_ref=pooled.at[source],
            send_sem=share_sem.at[0], recv_sem=share_sem.at[1],
            device_id=spot(worker), device_id_type=MESH,
        )

    for worker in range(workers):
        pl.when(me_plane != worker)(lambda worker=worker: pool_copy(me_plane, worker).start())

    def level_copy(step):
        return pltpu.make_async_remote_copy(
            src_ref=levels.at[0], dst_ref=levels.at[step],
            send_sem=share_sem.at[2], recv_sem=share_sem.at[3],
            device_id=beside(2, step), device_id_type=MESH,
        )

    def final_copy(worker, p):
        return pltpu.make_async_remote_copy(
            src_ref=final.at[pl.ds(worker * share, share)], dst_ref=final.at[pl.ds(worker * share, share)],
            send_sem=share_sem.at[4], recv_sem=share_sem.at[5],
            device_id=spot(p), device_id_type=MESH,
        )

    def pool():
        pooled[me_plane] = rows[mine]
        bulk(pooled.at[pl.ds(0, plane - 1)], share_sem.at[1]).wait()
        mean = added([pooled[p] for p in range(plane)]) / plane
        square = added([(pooled[p] - mean) * (pooled[p] - mean) for p in range(plane)])
        levels[0, 0] = mean
        levels[0, 1] = square
        for step in range(1, sizes[2]):
            level_copy(step).start()

    def merge():
        bulk(levels.at[pl.ds(0, sizes[2] - 1)], share_sem.at[3]).wait()
        heard = []
        for z in range(sizes[2]):
            at = lax.rem(place[2] - z + sizes[2], sizes[2])
            heard.append((levels[at, 0], levels[at, 1]))
        mean = added([part[0] for part in heard]) / sizes[2]
        square = added([part[1] for part in heard])
        apart = added([(part[0] - mean) * (part[0] - mean) for part in heard])
        square = square + plane * apart
        for w in range(share):
            final[me_plane * share + w, 0] = mean[w]
            final[me_plane * share + w, 1] = square[w]
        for p in range(plane):
            pl.when(me_plane != p)(lambda p=p: final_copy(me_plane, p).start())

    pl.when(works)(pool)
    for part in range(1, len(parts)):
        tail_copy(part).start()
    pl.when(works)(merge)
    pl.when(works)(lambda: bulk(final.at[pl.ds(0, (workers - 1) * share)], share_sem.at[5]).wait())
    pl.when(idles)(lambda: bulk(final.at[pl.ds(0, workers * share)], share_sem.at[5]).wait())

    def settled(r, mean, square):
        d, lanes = r // chunks, slice(r % chunks * cut, (r % chunks + 1) * cut)
        scale = sizes[d] / (2.0 * jnp.pi)
        centre_ref[d:d + 1, lanes] = -scale * mean
        spread_ref[d:d + 1, lanes] = scale * scale * (square / plan.devices)

    def norm(squares):
        return jnp.sum(jnp.sum(squares, axis=0, keepdims=True), axis=1, keepdims=True) / bands

    for r in range(plan.rows - 1):
        settled(r, final[r, 0], final[r, 1])
    coherence_ref[:, 0:1] = norm(xres[chunks:])
    coherence_ref[:, 1:2] = norm(total[y_slot])
    pl.when(works)(lambda: bulk(rows.at[pl.ds(0, (workers - 1) * share)], share_sem.at[0]).wait())
    pl.when(idles)(lambda: bulk(rows.at[pl.ds(0, workers * share)], share_sem.at[0]).wait())

    def settle():
        bulk(levels.at[pl.ds(0, sizes[2] - 1)], share_sem.at[2]).wait()
        bulk(final.at[pl.ds(0, (plane - 1) * share)], share_sem.at[4]).wait()

    pl.when(works)(settle)
    if plan.paired:
        pl.when(computes)(lambda: xres_copy.wait_send())
    when(yields, lambda: bulk(own, send_sem.at[0]).wait())
    bulk(own, send_sem.at[1]).wait()
    for part in range(len(parts) - 1):
        tail_copy(part).wait_recv()
        whole(z_slot, rolled.at[2], 2, last, parts[part])

    lanes = parts[-1]
    edge = bands - lanes[1]
    tail_copy(len(parts) - 1).wait_recv()
    measure(z_slot, rolled.at[2], 2, last, edge, lanes[1], lanes)
    every[me] = jnp.arctan2(-diag_im[z_slot, last:last + 1], diag_re[z_slot, last:last + 1])

    def place_of(k):
        return (k // sizes[1]) % sizes[0], k % sizes[1], k // plane

    def slot_of(k):
        x, y, z = place_of(k)
        return (x * sizes[1] + y) * sizes[2] + z

    def every_copy(k):
        x, y, z = place_of(k)
        return pltpu.make_async_remote_copy(
            src_ref=every.at[me], dst_ref=every.at[me],
            send_sem=every_sem.at[0], recv_sem=every_sem.at[1],
            device_id={"kx": x, "ky": y, "kz": z}, device_id_type=MESH,
        )

    few = plan.devices <= 64

    def each(act):
        def one(k, carry=0):
            pl.when(me != slot_of(k))(lambda: act(k))
            return carry
        if few:
            for k in range(plan.devices):
                one(k)
        else:
            lax.fori_loop(0, plan.devices, one, 0)

    each(lambda k: every_copy(k).start())
    for start in range(0, edge, ROWS):
        measure(z_slot, rolled.at[2], 2, last, start, min(ROWS, edge - start), lanes)
    ztotal_copy = pltpu.make_async_remote_copy(
        src_ref=total.at[z_slot], dst_ref=ztotal, send_sem=xres_sem.at[2], recv_sem=xres_sem.at[3],
        device_id=beside(2, sizes[2] - plan.toward[2]), device_id_type=MESH,
    )
    ztotal_copy.start()
    bulk(own, send_sem.at[2]).wait()
    others = every.at[pl.ds(0, plan.devices - 1)]
    bulk(others, every_sem.at[0]).wait()
    ztotal_copy.wait_send()
    ztotal_copy.wait_recv()
    coherence_ref[:, 2:3] = norm(ztotal[...])

    bulk(others, every_sem.at[1]).wait()
    if few:
        heard = [every[k] for k in range(plan.devices)]
        mean = added(heard) / plan.devices
        square = added([(phase - mean) * (phase - mean) for phase in heard])
    else:
        zero = jnp.zeros((1, cut), jnp.float32)
        mean = lax.fori_loop(0, plan.devices, lambda k, sofar: sofar + every[k], zero) / plan.devices
        square = lax.fori_loop(
            0, plan.devices, lambda k, sofar: sofar + (every[k] - mean) * (every[k] - mean), zero
        )
    settled(plan.rows - 1, mean, square)


def results(held_centre, held_spread, held_coherence, centre_ref, spread_ref, coherence_ref, sems):
    pairs = ((held_centre, centre_ref), (held_spread, spread_ref), (held_coherence, coherence_ref))
    copies = [pltpu.make_async_copy(held, out, sems.at[k]) for k, (held, out) in enumerate(pairs)]
    for copy in copies:
        copy.start()
    for copy in copies:
        copy.wait()


def solution(mesh):
    sizes = tuple(mesh.shape[axis] for axis in AXES)

    def shards(coefficients, shift_blocks):
        bands, width = coefficients.shape[4], coefficients.shape[5]
        plan = Plan(sizes, bands, width)
        chunks = plan.chunks
        vmem = pl.BlockSpec(memory_space=pltpu.VMEM)
        hbm = pl.BlockSpec(memory_space=pl.ANY)
        dma = pltpu.SemaphoreType.DMA
        padded = plan.plane * plan.share
        shapes = ((3, bands), (3, bands), (1, 3))
        held = pl.pallas_call(
            functools.partial(kernel, plan),
            out_shape=tuple(pltpu.VMEM(shape, jnp.float32) for shape in shapes),
            in_specs=[hbm, hbm],
            out_specs=(vmem, vmem, vmem),
            scratch_shapes=[
                pltpu.SMEM((3,), jnp.int32),
                pltpu.VMEM((2, bands, width), jnp.bfloat16),
                pltpu.VMEM((3, chunks, 2, LANES, width), jnp.bfloat16),
                pltpu.VMEM((3, 2, bands, width), jnp.bfloat16),
                pltpu.VMEM((plan.slots, chunks, LANES), jnp.float32),
                pltpu.VMEM((plan.slots, chunks, LANES), jnp.float32),
                pltpu.VMEM((plan.slots, 8, LANES), jnp.float32),
                pltpu.VMEM((chunks + 8, LANES), jnp.float32),
                pltpu.VMEM((chunks + 8, LANES), jnp.float32),
                pltpu.VMEM((8, LANES), jnp.float32),
                pltpu.VMEM((padded, 1, LANES), jnp.float32),
                pltpu.VMEM((plan.plane, plan.share, 1, LANES), jnp.float32),
                pltpu.VMEM((sizes[2], 2, plan.share, 1, LANES), jnp.float32),
                pltpu.VMEM((padded, 2, 1, LANES), jnp.float32),
                pltpu.VMEM((plan.devices, 1, LANES), jnp.float32),
                dma,
                dma((2,)),
                dma((3,)),
                dma((3, chunks + len(plan.parts) - 1)),
                dma((4,)),
                dma((6,)),
                dma((2,)),
                pltpu.SemaphoreType.REGULAR((4,)),
            ],
            compiler_params=pltpu.CompilerParams(
                collective_id=0, has_side_effects=True, vmem_limit_bytes=60 * 1024 * 1024
            ),
        )(shift_blocks, coefficients.reshape(2, bands, width))
        held = [pltpu.with_memory_space_constraint(array, pltpu.VMEM) for array in held]
        centre, spread, coherence = pl.pallas_call(
            results,
            out_shape=tuple(jax.ShapeDtypeStruct(shape, jnp.float32) for shape in shapes),
            in_specs=[vmem, vmem, vmem],
            out_specs=(hbm, hbm, hbm),
            scratch_shapes=[dma((3,))],
        )(*held)
        return centre, spread, coherence.reshape(3, 1, 1, 1)

    in_specs = (P(None, "kx", "ky", "kz", None, None), P())
    out_specs = (P(), P(), P(None, "kx", "ky", "kz"))
    return jax.shard_map(shards, mesh=mesh, in_specs=in_specs, out_specs=out_specs, check_vma=False)
```
